256 devices in a mesh: state: 8 (over z), act: 32 (over x, y, core).
Axes of the slice: x: 4, y: 4, z: 8, core: 2. Of those that a mesh axis runs over, the one named last changes fastest.
Arguments:
- state_features: bfloat16 [768, 2048], P('state', 'act'), may hold values from -6 to 6
- action_features: bfloat16 [768, 256, 2048], P('state', 'act'), may hold values from -240 to 240
- targets: float32 [768], P('state'), may hold values from -12 to 12
- w_hidden: bfloat16 [2048, 2048], replicated, may hold values from -0.125 to 0.125
- w_head: float32 [2048], replicated, may hold values from -7 to 7
Outputs:
- grad_hidden: float32 [2048, 2048], P(('state', 'act'))
- grad_head: float32 [2048], replicated
- log_partition: float32 [768], P('state')
- mean_loss: float32 [], replicated
The draws below stay inside these ranges and needn't reach their ends.
All inputs are finite; a program needn't handle non-finite values.
Results may differ from the reference program's by a relative error of at most 0.006.
Values may be sent and summed in bfloat16 or wider, within the bound.
A program may use at most 128 MiB of HBM per device.

```python
import jax
import jax.numpy as jnp
from jax import lax

D = 2048
STATES = 768
ACTIONS = 256


def head_base(key):
    return jnp.clip(jax.random.normal(jax.random.fold_in(key, 7), (D,), jnp.float32), -6.0, 6.0)


def head_scale():
    return 150.0


def draw_w_head(key, part):
    base = head_base(key)
    return base * (head_scale() / D)


def draw_action_features(key, part):
    noise = jnp.clip(jax.random.normal(jax.random.fold_in(key, 11), (STATES, ACTIONS, D), jnp.float32), -6.0, 6.0)
    base = head_base(key)
    base_rms = jnp.sqrt(jnp.mean(base * base))
    direction = base / base_rms
    picked_states = jax.random.randint(jax.random.fold_in(key, 13), (6,), 0, STATES)
    picked_actions = jax.random.randint(jax.random.fold_in(key, 17), (6,), 0, ACTIONS - 1)
    strength = jnp.array([0.7, 0.8, 0.9, 0.7, 0.8, 0.9], jnp.float32)
    fresh = noise[picked_states, picked_actions]
    upper = 20.0 * (strength[:, None] * direction[None, :] + jnp.sqrt(1.0 - strength * strength)[:, None] * fresh) / 6.0 * 6.0
    lower_strength = strength - 2.0 / (head_scale() * base_rms)
    lower = 20.0 * (lower_strength[:, None] * direction[None, :] + jnp.sqrt(1.0 - lower_strength * lower_strength)[:, None] * fresh)
    noise = noise.at[picked_states, picked_actions].set(upper)
    noise = noise.at[picked_states, picked_actions + 1].set(lower)
    return noise.astype(jnp.bfloat16)


def block_scale(stream_key, shape, split, smallest, largest):
    def one(position, parts):
        steps = jax.random.uniform(jax.random.fold_in(jax.random.fold_in(stream_key, 6), position), (parts,), jnp.float32, smallest / len(split), largest / len(split))
        return jnp.repeat(jnp.exp(steps), shape[position] // parts).reshape((-1,) + (1,) * (len(shape) - position - 1))

    factor_of = one(*split[0])
    for cut in split[1:]:
        factor_of = factor_of * one(*cut)
    return factor_of


def scatter_about(key, shape, scale, bound, shards=(), kind=jnp.bfloat16):
    values = scale * jax.random.normal(key, shape, jnp.float32)
    if shards:
        values = values * block_scale(key, shape, shards, -0.22, 0.18)
    return jnp.clip(values, -bound, bound).astype(kind)


def setup_inputs(seed: int = 0) -> dict:
    arg_keys = jax.random.split(jax.random.key(seed), 6)
    return {
        "state_features": scatter_about(arg_keys[0], (STATES, D), 1.0, 6.0, ((0, 8), (1, 32))),
        "action_features": draw_action_features(jax.random.fold_in(arg_keys[5], 71), 0),
        "targets": scatter_about(arg_keys[2], (STATES,), 2.0, 12.0, ((0, 8),), jnp.float32),
        "w_hidden": scatter_about(arg_keys[3], (D, D), D ** -0.5, 0.125),
        "w_head": draw_w_head(jax.random.fold_in(arg_keys[5], 71), 0),
    }


norm_epsilon = 1e-06
penalty_weight = 2.0

def reference(state_features, action_features, targets, w_hidden, w_head):
    blocks = STATES // 8

    def block_step(partial_value, block_index):
        grad_hidden, grad_head, loss_sum = partial_value
        state_block = lax.dynamic_slice_in_dim(state_features, block_index * 8, 8, 0)
        action_block = lax.dynamic_slice_in_dim(action_features, block_index * 8, 8, 0)
        target_block = lax.dynamic_slice_in_dim(targets, block_index * 8, 8, 0)
        mixture = state_block.astype(jnp.float32)[:, None, :] + action_block.astype(jnp.float32)
        normed = (mixture * lax.rsqrt(lax.optimization_barrier(jnp.mean(mixture * mixture, -1, keepdims=True)) + norm_epsilon)).astype(jnp.bfloat16)
        flat_rows = normed.reshape(-1, D)
        preact = jnp.dot(flat_rows, w_hidden, preferred_element_type=jnp.float32)
        sigmoid_pre = jax.nn.sigmoid(preact)
        head_input = flat_rows.astype(jnp.float32) + preact * sigmoid_pre
        scores = lax.optimization_barrier(jnp.sum(head_input * w_head, -1)).reshape(8, ACTIONS)
        row_max = lax.optimization_barrier(jnp.max(scores, -1, keepdims=True))
        log_part = row_max[:, 0] + jnp.log(lax.optimization_barrier(jnp.sum(jnp.exp(scores - row_max), -1)))
        softmax_weight = jnp.exp(scores - log_part[:, None])
        is_data = (jnp.arange(ACTIONS, dtype=jnp.int32) == 0)[None, :]
        bellman_gap = scores - target_block[:, None]
        score_grad = penalty_weight * softmax_weight + jnp.where(is_data, bellman_gap - penalty_weight, 0.0)
        loss_terms = jnp.where(is_data, penalty_weight * (log_part[:, None] - scores) + 0.5 * bellman_gap * bellman_gap, 0.0)
        grad_flat = score_grad.reshape(-1)
        grad_head = grad_head + lax.optimization_barrier(jnp.sum(grad_flat[:, None] * head_input, 0))
        back_grad = (grad_flat[:, None] * w_head * (sigmoid_pre + preact * sigmoid_pre * (1.0 - sigmoid_pre))).astype(jnp.bfloat16)
        grad_hidden = grad_hidden + lax.dot_general(flat_rows, back_grad, (((0,), (0,)), ((), ())), preferred_element_type=jnp.float32)
        return ((grad_hidden, grad_head, loss_sum + jnp.sum(loss_terms)), log_part)
    initial = (jnp.zeros((D, D), jnp.float32), jnp.zeros((D,), jnp.float32), jnp.zeros((), jnp.float32))
    (grad_hidden, grad_head, loss_sum), log_parts = lax.scan(block_step, initial, jnp.arange(blocks, dtype=jnp.int32))
    return (grad_hidden, grad_head, log_parts.reshape(STATES), loss_sum / STATES)
```

```python
import jax
import jax.numpy as jnp
from jax import lax
from jax.experimental import pallas as pl
from jax.experimental.pallas import tpu as pltpu
from jax.sharding import Mesh
from jax.sharding import PartitionSpec as P

Z, X, Y, C = "state", "act_0", "act_1", "act_2"
ACT = (X, Y, C)
STATE_ACT = (Z, X, Y, C)

norm_epsilon = 1e-06
penalty_weight = 2.0

F32 = jnp.float32
BF16 = jnp.bfloat16
STATES = 96
ACTIONS = 8
ROWS = STATES * ACTIONS
WIDTH = 2048
HALF = WIDTH // 2
CHUNK = 256
SUB = 32
AHEAD = 384
LAST = 256
VECTOR = HALF + 128


def remote(src, dst, send, recv, **target):
    return pltpu.make_async_remote_copy(
        src_ref=src,
        dst_ref=dst,
        send_sem=send,
        recv_sem=recv,
        device_id=target,
        device_id_type=pl.DeviceIdType.MESH,
    )


def kernel(
    state_ref,
    act_hbm,
    targets_ref,
    w_hbm,
    head_ref,
    grad_ref,
    grad_head_ref,
    lse_ref,
    loss_ref,
    w_buf,
    act_buf,
    state_pair,
    state_all,
    state_f32,
    normed,
    preact,
    head_in,
    slope,
    back,
    score_part,
    score_peer,
    score_grad,
    lse_all,
    vec_x,
    vec_y,
    vec_z,
    vec_c,
    gx,
    gy,
    gz,
    far_x,
    far_y,
    near_x,
    near_y,
    mid_x,
    mid_y,
    last_x,
    last_y,
    far_z,
    near_z,
    mid_z,
    last_z,
    total,
    total_peer,
    sem_in,
    pair_sem,
    state_sem,
    rows_sem,
    score_sem,
    lse_sem,
    vec_x_sem,
    vec_y_sem,
    vec_z_sem,
    vec_c_sem,
    far_sem,
    near_sem,
    mid_sem,
    last_sem,
    far_z_sem,
    near_z_sem,
    mid_z_sem,
    last_z_sem,
    total_sem,
):
    z, x, y, c = (lax.axis_index(name) for name in (Z, X, Y, C))
    other = 1 - c
    half = pl.ds(pl.multiple_of(c * HALF, HALF), HALF)
    other_half = pl.ds(pl.multiple_of(other * HALF, HALF), HALF)

    def at(axis, step):
        if axis == Z:
            return lax.rem(z + step + 8, 8)
        return lax.rem((x if axis == X else y) + step + 4, 4)

    act_in = [
        pltpu.make_async_copy(
            act_hbm.at[pl.ds(i * CHUNK, CHUNK)], act_buf.at[pl.ds(i * CHUNK, CHUNK)], sem_in.at[i]
        )
        for i in range(3)
    ]
    w_in = pltpu.make_async_copy(w_hbm.at[:, half], w_buf, sem_in.at[3])
    for copy in act_in:
        copy.start()
    w_in.start()

    barrier = pltpu.get_barrier_semaphore()
    plane = [(dx, dy) for dx in range(4) for dy in range(4) if dx or dy]

    def greet(**target):
        pl.semaphore_signal(barrier, inc=1, device_id=target, device_id_type=pl.DeviceIdType.MESH)

    greet(**{C: other})
    for dx, dy in plane:
        greet(**{X: at(X, dx), Y: at(Y, dy)})
    for dz in range(1, 8):
        greet(**{Z: at(Z, dz)})
    pl.semaphore_wait(barrier, 1 + len(plane) + 7)

    pair = remote(state_ref, state_pair, pair_sem.at[0], pair_sem.at[1], **{C: other})
    pair.start()
    pair.wait_recv()
    mine, theirs = state_ref[...].astype(F32), state_pair[...].astype(F32)
    low = jnp.where(c == 0, mine, theirs)
    high = jnp.where(c == 0, theirs, mine)
    state_all[0] = jnp.concatenate([low, high], axis=1).astype(BF16)
    state_out = [
        remote(
            state_all.at[0],
            state_all.at[dx * 4 + dy],
            state_sem.at[0, dx * 4 + dy],
            state_sem.at[1, dx * 4 + dy],
            **{X: at(X, dx), Y: at(Y, dy)},
        )
        for dx, dy in plane
    ]
    for copy in state_out:
        copy.start()
    for copy in state_out:
        copy.wait_recv()
    for j in range(16):
        slot = lax.rem(x - j // 4 + 4, 4) * 4 + lax.rem(y - j % 4 + 4, 4)
        state_f32[:, j * 128 : (j + 1) * 128] = state_all[slot].astype(F32)

    def rows_out(i):
        return remote(
            normed.at[pl.ds(i * CHUNK, CHUNK)],
            normed.at[pl.ds(ROWS + i * CHUNK, CHUNK)],
            rows_sem.at[0, i],
            rows_sem.at[1, i],
            **{C: other},
        )

    def normalise(t, carry):
        first = pl.multiple_of(t * 16, 16)
        pieces = [
            jnp.broadcast_to(state_f32[pl.ds(2 * t + i, 1), :], (8, WIDTH)) for i in range(2)
        ]
        mixture = jnp.concatenate(pieces, 0) + act_buf[pl.ds(first, 16), :].astype(F32)
        scale = lax.rsqrt(jnp.mean(mixture * mixture, -1, keepdims=True) + norm_epsilon)
        normed[pl.ds(first, 16), :] = (mixture * scale).astype(BF16)
        return carry

    for i in range(3):
        act_in[i].wait()
        lax.fori_loop(i * 16, (i + 1) * 16, normalise, 0, unroll=2)
        rows_out(i).start()

    lane8 = lax.broadcasted_iota(jnp.int32, (8, 128), 1)
    row8 = lax.broadcasted_iota(jnp.int32, (8, 128), 0)

    def pick(core):
        return (lane8 == row8 + core * 8)[None]

    def hidden(i, carry):
        base = pl.multiple_of(i * CHUNK, CHUNK)
        preact[...] = jnp.dot(
            normed[pl.ds(base, CHUNK), :], w_buf[...], preferred_element_type=F32
        )
        core = jnp.where(i < 3, c, other)
        mask = pick(core)

        def finish(t, inner):
            sub = pl.ds(pl.multiple_of(t * SUB, SUB), SUB)
            rows = pl.ds(pl.multiple_of(base + t * SUB, SUB), SUB)
            p = preact[sub, :]
            w = head_ref[:, half]
            g = jax.nn.sigmoid(p)
            pg = p * g
            h = normed[rows, half].astype(F32) + pg
            head_in[rows, :] = h
            slope[rows, :] = w * (g + pg * (1.0 - g))
            s = jnp.sum(h * w, -1, keepdims=True).reshape(SUB // 8, 8, 1)
            score_part[pl.ds(i * (CHUNK // 8) + t * (SUB // 8), SUB // 8), :] = jnp.sum(
                jnp.where(mask, s, 0.0), 1
            )
            return inner

        lax.fori_loop(0, CHUNK // SUB, finish, 0)
        return carry

    w_in.wait()
    lax.fori_loop(0, 3, hidden, 0)

    def hidden_peer(i, carry):
        rows_out(i - 3).wait_recv()
        return hidden(i, carry)

    lax.fori_loop(3, 6, hidden_peer, 0)

    score_part[pl.ds(0, STATES), :] = score_part[pl.ds(0, STATES), :] + score_part[
        pl.ds(STATES, STATES), :
    ]
    scores_out = remote(
        score_part.at[pl.ds(0, STATES)], score_peer, score_sem.at[0], score_sem.at[1], **{C: other}
    )
    scores_out.start()
    scores_out.wait_recv()
    scores = score_part[pl.ds(0, STATES), :] + score_peer[...]
    lane = lax.broadcasted_iota(jnp.int32, (STATES, 128), 1)
    row = lax.broadcasted_iota(jnp.int32, (STATES, 128), 0)
    valid = lane < 16
    eye = lane == row
    top = jnp.max(jnp.where(valid, scores, -jnp.inf), -1, keepdims=True)
    local = jnp.sum(jnp.where(valid, jnp.exp(scores - top), 0.0), -1, keepdims=True)
    lse_all[0] = jnp.sum(jnp.where(eye, top + jnp.log(local), 0.0), 0, keepdims=True)
    lse_out = [
        remote(
            lse_all.at[0],
            lse_all.at[dx * 4 + dy],
            lse_sem.at[0, dx * 4 + dy],
            lse_sem.at[1, dx * 4 + dy],
            **{X: at(X, dx), Y: at(Y, dy)},
        )
        for dx, dy in plane
    ]
    for copy in lse_out:
        copy.start()
    for copy in lse_out:
        copy.wait_recv()
    parts = [
        lse_all[lax.rem(x - j // 4 + 4, 4) * 4 + lax.rem(y - j % 4 + 4, 4)] for j in range(16)
    ]
    peak = parts[0]
    for part in parts[1:]:
        peak = jnp.maximum(peak, part)
    mass = jnp.exp(parts[0] - peak)
    for part in parts[1:]:
        mass = mass + jnp.exp(part - peak)
    lse_row = peak + jnp.log(mass)
    lse_ref[...] = lse_row[:, :STATES]
    lse = jnp.sum(jnp.where(eye, lse_row, 0.0), -1, keepdims=True)
    eye_states = lax.broadcasted_iota(jnp.int32, (STATES, STATES), 1) == lax.broadcasted_iota(
        jnp.int32, (STATES, STATES), 0
    )
    target = jnp.sum(jnp.where(eye_states, targets_ref[...], 0.0), -1, keepdims=True)
    data_lane = jnp.where((x == 0) & (y == 0), 0, -1)
    is_data = lane == data_lane
    gap = scores - target
    score_grad[...] = jnp.where(
        valid, penalty_weight * jnp.exp(scores - lse), 0.0
    ) + jnp.where(is_data, gap - penalty_weight, 0.0)
    loss_terms = jnp.where(is_data, penalty_weight * (lse - scores) + 0.5 * gap * gap, 0.0)
    loss_here = jnp.sum(jnp.sum(loss_terms, 0, keepdims=True), -1, keepdims=True)
    loss_here = jnp.where(c == 0, loss_here, 0.0)

    def backward(t, head_sum):
        rows = pl.ds(pl.multiple_of(t * SUB, SUB), SUB)
        own = t < ROWS // SUB
        core = jnp.where(own, c, other)
        states = pl.multiple_of((t - jnp.where(own, 0, ROWS // SUB)) * (SUB // 8), SUB // 8)
        pieces = []
        for i in range(SUB // 8):
            line = jnp.broadcast_to(score_grad[pl.ds(states + i, 1), :], (8, 128))
            pieces.append(
                jnp.sum(jnp.where(lane8 == row8 + core * 8, line, 0.0), -1, keepdims=True)
            )
        g = jnp.concatenate(pieces, 0)
        back[rows, :] = (g * slope[rows, :]).astype(BF16)
        return head_sum + jnp.sum((g * head_in[rows, :]).reshape(SUB // 8, 8, HALF), 0)

    head_sum = lax.fori_loop(
        0, 2 * ROWS // SUB, backward, jnp.zeros((8, HALF), F32), unroll=1
    )
    vec_x[0, :, :HALF] = jnp.sum(head_sum, 0, keepdims=True)
    vec_x[0, :, HALF:] = jnp.broadcast_to(loss_here, (1, 128))

    def vec_copies(axis, buf, sem, count):
        return [
            remote(buf.at[0], buf.at[d], sem.at[0, d], sem.at[1, d], **{axis: at(axis, d)})
            for d in range(1, count)
        ]

    def vec_sum(buf, me, count):
        result = buf[me]
        for q in range(1, count):
            result = result + buf[lax.rem(me - q + count, count)]
        return result

    vec_x_out = vec_copies(X, vec_x, vec_x_sem, 4)
    vec_y_out = vec_copies(Y, vec_y, vec_y_sem, 4)
    vec_z_out = vec_copies(Z, vec_z, vec_z_sem, 8)
    vec_c_out = remote(vec_c.at[0], vec_c.at[1], vec_c_sem.at[0], vec_c_sem.at[1], **{C: other})
    for copy in vec_x_out:
        copy.start()

    def vec_step_y():
        for copy in vec_x_out:
            copy.wait_recv()
        vec_y[0] = vec_sum(vec_x, x, 4)
        for copy in vec_y_out:
            copy.start()

    def vec_step_z():
        for copy in vec_y_out:
            copy.wait_recv()
        vec_z[0] = vec_sum(vec_y, y, 4)
        for copy in vec_z_out:
            copy.start()

    def vec_step_c():
        for copy in vec_z_out:
            copy.wait_recv()
        vec_c[0] = vec_sum(vec_z, z, 8)
        vec_c_out.start()

    def target_z(k):
        return lax.rem(z + jnp.where(lax.rem(k, 2) == 1, 4 - (k + 1) // 2, 4 + k // 2), 8)

    branches = (
        (0, X, Y, x, y, gx, far_x, near_x, mid_x, last_x),
        (1, Y, X, y, x, gy, far_y, near_y, mid_y, last_y),
    )

    def far_copies(k, b):
        i, axis, _, me, _, g, far, _, _, _ = branches[b]
        zz = target_z(k)
        opposite = at(axis, 2)
        return [
            remote(
                g.at[zz, opposite, pl.ds(2 * s, 2)],
                far.at[k, s],
                far_sem.at[0, i, k, s],
                far_sem.at[1, i, k, s],
                **{axis: at(axis, 1 - 2 * s)},
            )
            for s in range(2)
        ]

    def near_copies(k, b):
        i, axis, _, me, _, g, _, near, _, _ = branches[b]
        zz = target_z(k)
        return [
            remote(
                g.at[zz, at(axis, 1 - 2 * s)],
                near.at[k, s],
                near_sem.at[0, i, k, s],
                near_sem.at[1, i, k, s],
                **{axis: at(axis, 1 - 2 * s)},
            )
            for s in range(2)
        ]

    def mid_copies(k, b):
        i, _, axis, me, _, g, _, _, mid, _ = branches[b]
        zz = target_z(k)
        return [
            remote(
                g.at[zz, me, at(axis, d)],
                mid.at[k, d - 1],
                mid_sem.at[0, i, k, d - 1],
                mid_sem.at[1, i, k, d - 1],
                **{axis: at(axis, d)},
            )
            for d in range(1, 4)
        ]

    def last_copy(k, b):
        i, _, _, me, me2, g, _, _, _, last = branches[b]
        zz = target_z(k)
        return remote(
            g.at[zz, me, me2],
            last.at[k],
            last_sem.at[0, i, k],
            last_sem.at[1, i, k],
            **{Z: zz},
        )

    def block(k):
        zz = target_z(k)
        columns = pl.ds(pl.multiple_of(zz * 256, 256), 256)
        product = lax.dot_general(
            normed[:, columns],
            back[...],
            (((0,), (0,)), ((), ())),
            preferred_element_type=F32,
        ).astype(BF16)
        for i in range(4):
            for j in range(4):
                part = product[i * 64 + j * 16 : i * 64 + j * 16 + 16, :]
                gx[zz, i, j] = part[:, :AHEAD]
                gy[zz, j, i] = part[:, AHEAD : 2 * AHEAD]
                gz[zz, i, j] = part[:, 2 * AHEAD :]
        for b in range(2):
            for copy in far_copies(k, b):
                copy.start()

    def stage_near(k):
        zz = target_z(k)
        for b in range(2):
            _, axis, _, _, _, g, far, _, _, _ = branches[b]
            for s, arrived in enumerate(far_copies(k, b)):
                arrived.wait_recv()
                slot = at(axis, 1 - 2 * s)
                ref = g.at[zz, slot, pl.ds(2 * s, 2)]
                ref[...] = (ref[...].astype(F32) + far[k, s].astype(F32)).astype(BF16)
            for copy in near_copies(k, b):
                copy.start()

    def stage_mid(k):
        zz = target_z(k)
        for b in range(2):
            _, _, _, me, _, g, _, near, _, _ = branches[b]
            for copy in near_copies(k, b):
                copy.wait_recv()
            g[zz, me] = (
                g[zz, me].astype(F32) + near[k, 0].astype(F32) + near[k, 1].astype(F32)
            ).astype(BF16)
            for copy in mid_copies(k, b):
                copy.start()

    def mid_total(k, b):
        _, _, _, me, me2, g, _, _, mid, _ = branches[b]
        for copy in mid_copies(k, b):
            copy.wait_recv()
        result = g[target_z(k), me, me2].astype(F32)
        for d in range(3):
            result = result + mid[k, d].astype(F32)
        return result

    def stage_last(k):
        zz = target_z(k)
        for b in range(2):
            _, _, _, me, me2, g, _, _, _, _ = branches[b]
            g[zz, me, me2] = mid_total(k, b).astype(BF16)
            last_copy(k, b).start()

    far_z_out = [
        remote(
            gz.at[at(Z, 4), pl.ds(2 * s, 2)],
            far_z.at[s],
            far_z_sem.at[0, s],
            far_z_sem.at[1, s],
            **{Z: at(Z, 1 - 2 * s)},
        )
        for s in range(2)
    ]

    def near_z_copy(j, s):
        return remote(
            gz.at[at(Z, j * (1 - 2 * s))],
            near_z.at[s, j - 1],
            near_z_sem.at[0, s, j - 1],
            near_z_sem.at[1, s, j - 1],
            **{Z: at(Z, 1 - 2 * s)},
        )

    def stage_z(j):
        for s in range(2):
            slot = at(Z, j * (1 - 2 * s))
            if j == 3:
                far_z_out[s].wait_recv()
                ref = gz.at[slot, pl.ds(2 * s, 2)]
                ref[...] = (ref[...].astype(F32) + far_z[s].astype(F32)).astype(BF16)
            else:
                near_z_copy(j + 1, s).wait_recv()
                gz[slot] = (gz[slot].astype(F32) + near_z[s, j].astype(F32)).astype(BF16)
            near_z_copy(j, s).start()

    mid_z_out = [
        remote(
            gz.at[z, at(X, d)],
            mid_z.at[d - 1],
            mid_z_sem.at[0, d - 1],
            mid_z_sem.at[1, d - 1],
            **{X: at(X, d)},
        )
        for d in range(1, 4)
    ]
    last_z_out = [
        remote(
            gz.at[z, x, at(Y, d)],
            last_z.at[d - 1],
            last_z_sem.at[0, d - 1],
            last_z_sem.at[1, d - 1],
            **{Y: at(Y, d)},
        )
        for d in range(1, 4)
    ]

    def stage_z_mid():
        for s in range(2):
            near_z_copy(1, s).wait_recv()
        gz[z] = (
            gz[z].astype(F32) + near_z[0, 0].astype(F32) + near_z[1, 0].astype(F32)
        ).astype(BF16)
        for copy in mid_z_out:
            copy.start()

    def stage_z_last():
        for copy in mid_z_out:
            copy.wait_recv()
        sums = gz[z, x].astype(F32)
        for d in range(3):
            sums = sums + mid_z[d].astype(F32)
        gz[z, x] = sums.astype(BF16)
        for copy in last_z_out:
            copy.start()

    def step(t, carry):
        @pl.when(t < 8)
        def _():
            block(t)

        @pl.when(t == 0)
        def _():
            for copy in far_z_out:
                copy.start()

        for when, j in ((3, 3), (6, 2), (8, 1)):

            @pl.when(t == when)
            def _(j=j):
                stage_z(j)

        @pl.when((t >= 2) & (t < 10))
        def _():
            stage_near(t - 2)

        @pl.when((t >= 4) & (t < 12))
        def _():
            stage_mid(t - 4)

        @pl.when((t >= 6) & (t < 13))
        def _():
            stage_last(t - 6)

        for when, part in (
            (2, vec_step_y),
            (5, vec_step_z),
            (7, vec_step_c),
            (10, stage_z_mid),
            (12, stage_z_last),
        ):

            @pl.when(t == when)
            def _(part=part):
                part()

        return carry

    lax.fori_loop(0, 13, step, 0)

    for b in range(2):
        last = branches[b][9]
        result = mid_total(7, b)
        for k in range(7):
            last_copy(k, b).wait_recv()
            result = result + last[k].astype(F32)
        for i in range(2):
            total[i, :, b * AHEAD : (b + 1) * AHEAD] = result[8 * i : 8 * i + 8, :]
    for copy in last_z_out:
        copy.wait_recv()
    result = gz[z, x, y].astype(F32)
    for d in range(3):
        result = result + last_z[d].astype(F32)
    for i in range(2):
        total[i, :, 2 * AHEAD :] = result[8 * i : 8 * i + 8, :]
    total_out = remote(
        total.at[other], total_peer, total_sem.at[0], total_sem.at[1], **{C: other}
    )
    total_out.start()

    vec_c_out.wait_recv()
    grad_head_ref[:, half] = vec_c[0, :, :HALF]
    grad_head_ref[:, other_half] = vec_c[1, :, :HALF]
    loss_ref[...] = (vec_c[0, :, HALF:] + vec_c[1, :, HALF:]) * (1.0 / (STATES * 8))
    grad_ref[:, half] = total[c]

    sent = [pair, scores_out, vec_c_out]
    sent += state_out + lse_out + vec_x_out + vec_y_out + vec_z_out
    sent += far_z_out + mid_z_out + last_z_out
    sent += [rows_out(i) for i in range(3)]
    sent += [near_z_copy(j, s) for j in range(1, 4) for s in range(2)]
    for copy in sent:
        copy.wait_send()

    def drain(k, carry):
        for b in range(2):
            for copy in far_copies(k, b) + near_copies(k, b) + mid_copies(k, b):
                copy.wait_send()

            @pl.when(k < 7)
            def _(b=b):
                last_copy(k, b).wait_send()

        return carry

    lax.fori_loop(0, 8, drain, 0)
    total_out.wait()
    grad_ref[:, other_half] = total_peer[...]


def body(state_features, action_features, targets, w_hidden, w_head):
    vmem = pl.BlockSpec(memory_space=pltpu.VMEM)
    anywhere = pl.BlockSpec(memory_space=pl.ANY)
    dma = pltpu.SemaphoreType.DMA
    scratch = [
        pltpu.VMEM((WIDTH, HALF), BF16),
        pltpu.VMEM((ROWS, WIDTH), BF16),
        pltpu.VMEM((STATES, 64), BF16),
        pltpu.VMEM((16, STATES, 128), BF16),
        pltpu.VMEM((STATES, WIDTH), F32),
        pltpu.VMEM((2 * ROWS, WIDTH), BF16),
        pltpu.VMEM((CHUNK, HALF), F32),
        pltpu.VMEM((2 * ROWS, HALF), F32),
        pltpu.VMEM((2 * ROWS, HALF), F32),
        pltpu.VMEM((2 * ROWS, HALF), BF16),
        pltpu.VMEM((2 * STATES, 128), F32),
        pltpu.VMEM((STATES, 128), F32),
        pltpu.VMEM((STATES, 128), F32),
        pltpu.VMEM((16, 1, 128), F32),
        pltpu.VMEM((4, 1, VECTOR), F32),
        pltpu.VMEM((4, 1, VECTOR), F32),
        pltpu.VMEM((8, 1, VECTOR), F32),
        pltpu.VMEM((2, 1, VECTOR), F32),
        pltpu.VMEM((8, 4, 4, 16, AHEAD), BF16),
        pltpu.VMEM((8, 4, 4, 16, AHEAD), BF16),
        pltpu.VMEM((8, 4, 4, 16, LAST), BF16),
        pltpu.VMEM((8, 2, 2, 16, AHEAD), BF16),
        pltpu.VMEM((8, 2, 2, 16, AHEAD), BF16),
        pltpu.VMEM((8, 2, 4, 16, AHEAD), BF16),
        pltpu.VMEM((8, 2, 4, 16, AHEAD), BF16),
        pltpu.VMEM((8, 3, 16, AHEAD), BF16),
        pltpu.VMEM((8, 3, 16, AHEAD), BF16),
        pltpu.VMEM((8, 16, AHEAD), BF16),
        pltpu.VMEM((8, 16, AHEAD), BF16),
        pltpu.VMEM((2, 2, 4, 16, LAST), BF16),
        pltpu.VMEM((2, 3, 4, 4, 16, LAST), BF16),
        pltpu.VMEM((3, 4, 16, LAST), BF16),
        pltpu.VMEM((3, 16, LAST), BF16),
        pltpu.VMEM((2, 8, HALF), F32),
        pltpu.VMEM((8, HALF), F32),
        dma((4,)),
        dma((2,)),
        dma((2, 16)),
        dma((2, 3)),
        dma((2,)),
        dma((2, 16)),
        dma((2, 4)),
        dma((2, 4)),
        dma((2, 8)),
        dma((2,)),
        dma((2, 2, 8, 2)),
        dma((2, 2, 8, 2)),
        dma((2, 2, 8, 3)),
        dma((2, 2, 8)),
        dma((2, 2)),
        dma((2, 2, 3)),
        dma((2, 3)),
        dma((2, 3)),
        dma((2,)),
    ]
    grad, grad_head, lse, loss = pl.pallas_call(
        kernel,
        out_shape=(
            jax.ShapeDtypeStruct((8, WIDTH), F32),
            jax.ShapeDtypeStruct((1, WIDTH), F32),
            jax.ShapeDtypeStruct((1, STATES), F32),
            jax.ShapeDtypeStruct((1, 128), F32),
        ),
        in_specs=[vmem, anywhere, vmem, anywhere, vmem],
        out_specs=(vmem,) * 4,
        scratch_shapes=scratch,
        compiler_params=pltpu.CompilerParams(
            collective_id=0, has_side_effects=True, vmem_limit_bytes=62 * 1024 * 1024
        ),
        name="critic",
    )(
        state_features,
        action_features.reshape(ROWS, WIDTH),
        targets.reshape(1, STATES),
        w_hidden,
        w_head.reshape(1, WIDTH),
    )
    return grad, grad_head.reshape(WIDTH), lse.reshape(STATES), loss[0, 0]


def solution(mesh):
    finer = Mesh(mesh.devices.reshape(8, 4, 4, 2), (Z, X, Y, C))
    return jax.shard_map(
        body,
        mesh=finer,
        in_specs=(P(Z, ACT), P(Z, ACT, None), P(Z), P(), P()),
        out_specs=(P(STATE_ACT, None), P(), P(Z), P()),
        check_vma=False,
    )
```

```python
import jax
import jax.numpy as jnp
from jax import lax
from jax.experimental import pallas as pl
from jax.experimental.pallas import tpu as pltpu
from jax.sharding import Mesh
from jax.sharding import PartitionSpec as P

Z, X, Y, C = "state", "act_0", "act_1", "act_2"
ACT = (X, Y, C)
STATE_ACT = (Z, X, Y, C)

norm_epsilon = 1e-06
penalty_weight = 2.0

F32 = jnp.float32
BF16 = jnp.bfloat16
STATES = 96
ACTIONS = 8
ROWS = STATES * ACTIONS
WIDTH = 2048
HALF = WIDTH // 2
CHUNK = 256
SUB = 32
AHEAD = 384
LAST = 256
VECTOR = HALF + 128
GROUPS = ((0,), (1, 2), (3, 4), (5, 6), (7,))
DEPTH = 2
PLUS = {4: 0, 3: 1, 2: 3, 1: 5}
MINUS = {3: 2, 2: 4, 1: 6}


def remote(src, dst, send, recv, **target):
    return pltpu.make_async_remote_copy(
        src_ref=src,
        dst_ref=dst,
        send_sem=send,
        recv_sem=recv,
        device_id=target,
        device_id_type=pl.DeviceIdType.MESH,
    )


def kernel(
    state_ref,
    act_hbm,
    targets_ref,
    w_hbm,
    head_ref,
    grad_ref,
    grad_head_ref,
    lse_ref,
    loss_ref,
    w_buf,
    act_buf,
    state_own,
    state_all,
    state_f32,
    normed,
    preact_a,
    preact_b,
    head_in,
    slope,
    back,
    score_lanes,
    score_part,
    score_peer,
    score_grad,
    grad_rows,
    lse_all,
    vec_x,
    vec_y,
    vec_z,
    vec_c,
    gx,
    gy,
    gz,
    far_x,
    far_y,
    near_x,
    near_y,
    mid_x,
    mid_y,
    last_x,
    last_y,
    far_z,
    near_z,
    plane_z,
    total,
    total_peer,
    sem_in,
    pair_sem,
    state_sem,
    rows_sem,
    score_sem,
    lse_sem,
    vec_x_sem,
    vec_y_sem,
    vec_z_sem,
    vec_c_sem,
    far_sem,
    near_sem,
    mid_sem,
    last_sem,
    far_z_sem,
    near_z_sem,
    plane_z_sem,
    total_sem,
):
    z, x, y, c = (lax.axis_index(name) for name in (Z, X, Y, C))
    other = 1 - c
    half = pl.ds(pl.multiple_of(c * HALF, HALF), HALF)
    other_half = pl.ds(pl.multiple_of(other * HALF, HALF), HALF)

    def at(axis, step):
        if axis == Z:
            return lax.rem(z + step + 8, 8)
        return lax.rem((x if axis == X else y) + step + 4, 4)

    act_in = [
        pltpu.make_async_copy(
            act_hbm.at[pl.ds(i * CHUNK, CHUNK)], act_buf.at[pl.ds(i * CHUNK, CHUNK)], sem_in.at[i]
        )
        for i in range(3)
    ]
    w_in = pltpu.make_async_copy(w_hbm.at[:, half], w_buf, sem_in.at[3])
    for copy in act_in:
        copy.start()
    w_in.start()

    barrier = pltpu.get_barrier_semaphore()
    plane = [(dx, dy) for dx in range(4) for dy in range(4) if dx or dy]

    def greet(**target):
        pl.semaphore_signal(barrier, inc=1, device_id=target, device_id_type=pl.DeviceIdType.MESH)

    greet(**{C: other})
    for dx, dy in plane:
        greet(**{X: at(X, dx), Y: at(Y, dy)})
    for dz in range(1, 8):
        greet(**{Z: at(Z, dz)})
    pl.semaphore_wait(barrier, 1 + len(plane) + 7)

    state_own[...] = jnp.zeros(state_own.shape, BF16)
    state_own[:, :STATES] = state_ref[...]
    state_all[c, 0] = state_own[...]
    state_out = [
        remote(
            state_own,
            state_all.at[c, dx * 4 + dy],
            state_sem.at[0, dx * 4 + dy],
            state_sem.at[1, dx * 4 + dy],
            **{X: at(X, dx), Y: at(Y, dy)},
        )
        for dx, dy in plane
    ]
    for copy in state_out:
        copy.start()
    for copy in state_out:
        copy.wait_recv()
    pair = remote(state_all.at[c], state_all.at[c], pair_sem.at[0], pair_sem.at[1], **{C: other})
    pair_in = remote(
        state_all.at[other], state_all.at[other], pair_sem.at[0], pair_sem.at[1], **{C: other}
    )
    pair.start()
    pair_in.wait_recv()
    for j in range(16):
        slot = lax.rem(x - j // 4 + 4, 4) * 4 + lax.rem(y - j % 4 + 4, 4)
        tile = jnp.concatenate([state_all[0, slot], state_all[1, slot]], 0).astype(F32)
        state_f32[:, j * 128 : (j + 1) * 128] = tile.T[:STATES, :]

    def rows_out(i):
        return remote(
            normed.at[pl.ds(i * CHUNK, CHUNK)],
            normed.at[pl.ds(ROWS + i * CHUNK, CHUNK)],
            rows_sem.at[0, i],
            rows_sem.at[1, i],
            **{C: other},
        )

    def mixture(u, j):
        tile = slice(j * 128, (j + 1) * 128)
        lines = state_f32[u * 8 : u * 8 + 8, tile]
        lines = jnp.broadcast_to(lines[:, None, :], (8, 8, 128)).reshape(64, 128)
        return lines + act_buf[u * 64 : u * 64 + 64, tile].astype(F32)

    def normalise(i):
        act_in[i].wait()
        for u in range(i * 4, i * 4 + 4):
            rows = slice(u * 64, u * 64 + 64)
            sums = None
            for j in range(WIDTH // 128):
                m = mixture(u, j)
                sums = m * m if sums is None else sums + m * m
            mean = jnp.sum(sums, -1, keepdims=True) * (1.0 / WIDTH)
            factor = jnp.broadcast_to(lax.rsqrt(mean + norm_epsilon), (64, 128))
            for j in range(WIDTH // 128):
                normed[rows, j * 128 : (j + 1) * 128] = (mixture(u, j) * factor).astype(BF16)

    lane8 = lax.broadcasted_iota(jnp.int32, (8, 128), 1)
    row8 = lax.broadcasted_iota(jnp.int32, (8, 128), 0)

    def product(i, buf):
        buf[...] = jnp.dot(
            normed[i * CHUNK : (i + 1) * CHUNK, :], w_buf[...], preferred_element_type=F32
        )

    def finish(i, buf):
        w = head_ref[:, half]
        for t in range(CHUNK // SUB):
            rows = slice(i * CHUNK + t * SUB, i * CHUNK + (t + 1) * SUB)
            p = buf[t * SUB : (t + 1) * SUB, :]
            g = 0.5 * jnp.tanh(0.5 * p) + 0.5
            pg = p * g
            h = normed[rows, half].astype(F32) + pg
            head_in[rows, :] = h
            slope[rows, :] = w * (g + pg * (1.0 - g))
            hw = h * w
            sums = hw[:, :128]
            for j in range(1, HALF // 128):
                sums = sums + hw[:, j * 128 : (j + 1) * 128]
            score_lanes[rows, :] = sums

    buffers = (preact_a, preact_b)
    normalise(0)
    rows_out(0).start()
    w_in.wait()
    for i in range(6):
        if i >= 3:
            rows_out(i - 3).wait_recv()
        product(i, buffers[i % 2])
        if i < 2:
            normalise(i + 1)
            rows_out(i + 1).start()
        if i > 0:
            finish(i - 1, buffers[(i - 1) % 2])
    finish(5, buffers[1])

    for i in range(3):
        states = 0.0
        for part, core in ((0, c), (1, other)):
            first = part * ROWS + i * CHUNK
            column = jnp.sum(score_lanes[first : first + CHUNK, :], -1, keepdims=True)
            column = column.reshape(CHUNK // 8, 8, 1)
            states = states + jnp.sum(
                jnp.where((lane8 == row8 + core * 8)[None], column, 0.0), 1
            )
        score_part[i * (CHUNK // 8) : (i + 1) * (CHUNK // 8), :] = states
    scores_out = remote(score_part, score_peer, score_sem.at[0], score_sem.at[1], **{C: other})
    scores_out.start()
    scores_out.wait_recv()
    scores = score_part[...] + score_peer[...]
    lane = lax.broadcasted_iota(jnp.int32, (STATES, 128), 1)
    row = lax.broadcasted_iota(jnp.int32, (STATES, 128), 0)
    valid = lane < 16
    eye = lane == row
    top = jnp.max(jnp.where(valid, scores, -jnp.inf), -1, keepdims=True)
    local = jnp.sum(jnp.where(valid, jnp.exp(scores - top), 0.0), -1, keepdims=True)
    lse_all[0] = jnp.sum(jnp.where(eye, top + jnp.log(local), 0.0), 0, keepdims=True)
    lse_out = [
        remote(
            lse_all.at[0],
            lse_all.at[dx * 4 + dy],
            lse_sem.at[0, dx * 4 + dy],
            lse_sem.at[1, dx * 4 + dy],
            **{X: at(X, dx), Y: at(Y, dy)},
        )
        for dx, dy in plane
    ]
    for copy in lse_out:
        copy.start()
    for copy in lse_out:
        copy.wait_recv()
    parts = [
        lse_all[lax.rem(x - j // 4 + 4, 4) * 4 + lax.rem(y - j % 4 + 4, 4)] for j in range(16)
    ]
    peak = parts[0]
    for part in parts[1:]:
        peak = jnp.maximum(peak, part)
    mass = jnp.exp(parts[0] - peak)
    for part in parts[1:]:
        mass = mass + jnp.exp(part - peak)
    lse_row = peak + jnp.log(mass)
    lse_ref[...] = lse_row[:, :STATES]
    lse = jnp.sum(jnp.where(eye, lse_row, 0.0), -1, keepdims=True)
    eye_states = lax.broadcasted_iota(jnp.int32, (STATES, STATES), 1) == lax.broadcasted_iota(
        jnp.int32, (STATES, STATES), 0
    )
    target = jnp.sum(jnp.where(eye_states, targets_ref[...], 0.0), -1, keepdims=True)
    data_lane = jnp.where((x == 0) & (y == 0), 0, -1)
    is_data = lane == data_lane
    gap = scores - target
    score_grad[...] = jnp.where(
        valid, penalty_weight * jnp.exp(scores - lse), 0.0
    ) + jnp.where(is_data, gap - penalty_weight, 0.0)
    loss_terms = jnp.where(is_data, penalty_weight * (lse - scores) + 0.5 * gap * gap, 0.0)
    loss_here = jnp.sum(jnp.sum(loss_terms, 0, keepdims=True), -1, keepdims=True)
    loss_here = jnp.where(c == 0, loss_here, 0.0)

    for part, core in ((0, c), (1, other)):
        for i in range(3):
            lines = score_grad[i * (CHUNK // 8) : (i + 1) * (CHUNK // 8), :]
            lines = jnp.broadcast_to(lines[:, None, :], (CHUNK // 8, 8, 128))
            lines = jnp.where((lane8 == row8 + core * 8)[None], lines, 0.0)
            column = jnp.sum(lines.reshape(CHUNK, 128), -1, keepdims=True)
            first = part * ROWS + i * CHUNK
            grad_rows[first : first + CHUNK, :] = jnp.broadcast_to(column, (CHUNK, 128))

    def backward(t, head_sum):
        rows = pl.ds(pl.multiple_of(t * SUB, SUB), SUB)
        g = jnp.concatenate([grad_rows[rows, :]] * (HALF // 128), 1)
        back[rows, :] = (g * slope[rows, :]).astype(BF16)
        return head_sum + jnp.sum((g * head_in[rows, :]).reshape(SUB // 8, 8, HALF), 0)

    head_sum = lax.fori_loop(0, 2 * ROWS // SUB, backward, jnp.zeros((8, HALF), F32), unroll=2)
    vec_x[0, :, :HALF] = jnp.sum(head_sum, 0, keepdims=True)
    vec_x[0, :, HALF:] = jnp.broadcast_to(loss_here, (1, 128))

    def vec_copies(axis, buf, sem, count):
        return [
            remote(buf.at[0], buf.at[d], sem.at[0, d], sem.at[1, d], **{axis: at(axis, d)})
            for d in range(1, count)
        ]

    def vec_sum(buf, me, count):
        result = buf[me]
        for q in range(1, count):
            result = result + buf[lax.rem(me - q + count, count)]
        return result

    vec_x_out = vec_copies(X, vec_x, vec_x_sem, 4)
    vec_y_out = vec_copies(Y, vec_y, vec_y_sem, 4)
    vec_z_out = vec_copies(Z, vec_z, vec_z_sem, 8)
    vec_c_out = remote(vec_c.at[0], vec_c.at[1], vec_c_sem.at[0], vec_c_sem.at[1], **{C: other})
    for copy in vec_x_out:
        copy.start()

    def vec_step_y():
        for copy in vec_x_out:
            copy.wait_recv()
        vec_y[0] = vec_sum(vec_x, x, 4)
        for copy in vec_y_out:
            copy.start()

    def vec_step_z():
        for copy in vec_y_out:
            copy.wait_recv()
        vec_z[0] = vec_sum(vec_y, y, 4)
        for copy in vec_z_out:
            copy.start()

    def vec_step_c():
        for copy in vec_z_out:
            copy.wait_recv()
        vec_c[0] = vec_sum(vec_z, z, 8)
        vec_c_out.start()

    def target_z(k):
        return lax.rem(z + jnp.where(lax.rem(k, 2) == 1, 4 - (k + 1) // 2, 4 + k // 2), 8)

    branches = (
        (0, X, Y, x, y, gx, far_x, near_x, mid_x, last_x),
        (1, Y, X, y, x, gy, far_y, near_y, mid_y, last_y),
    )

    def held(n):
        return pl.ds(0, len(GROUPS[n]))

    def far_copies(n, b):
        i, axis, _, me, _, g, far, _, _, _ = branches[b]
        return [
            remote(
                g.at[n, at(axis, 2), pl.ds(2 * s, 2), held(n)],
                far.at[n, s, :, held(n)],
                far_sem.at[0, i, n, s],
                far_sem.at[1, i, n, s],
                **{axis: at(axis, 1 - 2 * s)},
            )
            for s in range(2)
        ]

    def near_copies(n, b):
        i, axis, _, me, _, g, _, near, _, _ = branches[b]
        return [
            remote(
                g.at[n, at(axis, 1 - 2 * s), :, held(n)],
                near.at[n, s, :, held(n)],
                near_sem.at[0, i, n, s],
                near_sem.at[1, i, n, s],
                **{axis: at(axis, 1 - 2 * s)},
            )
            for s in range(2)
        ]

    def mid_copies(n, b):
        i, _, axis, me, _, g, _, _, mid, _ = branches[b]
        return [
            remote(
                g.at[n, me, at(axis, d), held(n)],
                mid.at[n, d - 1, held(n)],
                mid_sem.at[0, i, n, d - 1],
                mid_sem.at[1, i, n, d - 1],
                **{axis: at(axis, d)},
            )
            for d in range(1, 4)
        ]

    def last_copy(k, b):
        i, _, _, me, me2, g, _, _, _, last = branches[b]
        return remote(
            g.at[(k + 1) // 2, me, me2, 0 if k == 0 else (k + 1) % 2],
            last.at[k],
            last_sem.at[0, i, k],
            last_sem.at[1, i, k],
            **{Z: target_z(k)},
        )

    def block(n, d):
        k = GROUPS[n][0] + d
        columns = pl.ds(pl.multiple_of(target_z(k) * 256, 256), 256)
        result = lax.dot_general(
            normed[:, columns],
            back[...],
            (((0,), (0,)), ((), ())),
            preferred_element_type=F32,
        ).astype(BF16)
        for i in range(4):
            for j in range(4):
                part = result[i * 64 + j * 16 : i * 64 + j * 16 + 16, :]
                gx[n, i, j, d] = part[:, :AHEAD]
                gy[n, j, i, d] = part[:, AHEAD : 2 * AHEAD]
                gz[k, i, j] = part[:, 2 * AHEAD :]

    def stage_block(n):
        def one(d, carry):
            block(n, d)
            return carry

        lax.fori_loop(0, len(GROUPS[n]), one, 0)
        for b in range(2):
            for copy in far_copies(n, b):
                copy.start()

    def stage_near(n):
        for b in range(2):
            _, axis, _, _, _, g, far, _, _, _ = branches[b]
            copies = near_copies(n, b)
            for s, arrived in enumerate(far_copies(n, b)):
                arrived.wait_recv()
                ref = g.at[n, at(axis, 1 - 2 * s), pl.ds(2 * s, 2), held(n)]
                ref[...] = (
                    ref[...].astype(F32) + far[n, s, :, held(n)].astype(F32)
                ).astype(BF16)
                copies[s].start()

    def stage_mid(n):
        for b in range(2):
            _, _, _, me, _, g, _, near, _, _ = branches[b]
            for copy in near_copies(n, b):
                copy.wait_recv()
            ref = g.at[n, me, :, held(n)]
            ref[...] = (
                ref[...].astype(F32)
                + near[n, 0, :, held(n)].astype(F32)
                + near[n, 1, :, held(n)].astype(F32)
            ).astype(BF16)
            for copy in mid_copies(n, b):
                copy.start()

    def mid_total(n, b):
        _, _, _, me, me2, g, _, _, mid, _ = branches[b]
        for copy in mid_copies(n, b):
            copy.wait_recv()
        result = g[n, me, me2, held(n)].astype(F32)
        for d in range(3):
            result = result + mid[n, d, held(n)].astype(F32)
        return result

    def stage_last(n):
        for b in range(2):
            _, _, _, me, me2, g, _, _, _, _ = branches[b]
            g[n, me, me2, held(n)] = mid_total(n, b).astype(BF16)
            for k in GROUPS[n]:
                last_copy(k, b).start()

    far_z_out = [
        remote(
            gz.at[PLUS[4], pl.ds(2 * s, 2)],
            far_z.at[s],
            far_z_sem.at[0, s],
            far_z_sem.at[1, s],
            **{Z: at(Z, 1 - 2 * s)},
        )
        for s in range(2)
    ]

    def near_z_copy(j, s, h):
        return remote(
            gz.at[(PLUS, MINUS)[s][j], pl.ds(2 * h, 2)],
            near_z.at[s, j - 1, pl.ds(2 * h, 2)],
            near_z_sem.at[0, s, j - 1, h],
            near_z_sem.at[1, s, j - 1, h],
            **{Z: at(Z, 1 - 2 * s)},
        )

    def stage_z(j, late):
        for s in range(2):
            h = s if late else 1 - s
            ref = gz.at[(PLUS, MINUS)[s][j], pl.ds(2 * h, 2)]
            arrived = None
            if j < 3:
                near_z_copy(j + 1, s, h).wait_recv()
                arrived = near_z[s, j, pl.ds(2 * h, 2)]
            elif late:
                far_z_out[s].wait_recv()
                arrived = far_z[s]
            if arrived is not None:
                ref[...] = (ref[...].astype(F32) + arrived.astype(F32)).astype(BF16)
            near_z_copy(j, s, h).start()

    plane_z_out = [
        remote(
            gz.at[7, at(X, dx), at(Y, dy)],
            plane_z.at[dx * 4 + dy],
            plane_z_sem.at[0, dx * 4 + dy],
            plane_z_sem.at[1, dx * 4 + dy],
            **{X: at(X, dx), Y: at(Y, dy)},
        )
        for dx, dy in plane
    ]

    def stage_z_plane():
        for s in range(2):
            for h in range(2):
                near_z_copy(1, s, h).wait_recv()
        gz[7] = (
            gz[7].astype(F32) + near_z[0, 0].astype(F32) + near_z[1, 0].astype(F32)
        ).astype(BF16)
        for copy in plane_z_out:
            copy.start()

    stage_block(0)
    for copy in far_z_out:
        copy.start()
    stage_block(1)
    stage_z(3, 0)
    stage_block(2)
    vec_step_y()
    stage_near(0)
    stage_z(3, 1)
    stage_block(3)
    stage_block(4)
    stage_near(1)
    stage_z(2, 0)
    stage_near(2)
    stage_z(2, 1)
    stage_mid(0)
    vec_step_z()
    stage_near(3)
    stage_near(4)
    stage_z(1, 0)
    stage_mid(1)
    stage_z(1, 1)
    stage_mid(2)
    stage_last(0)
    vec_step_c()
    stage_mid(3)
    stage_last(1)
    stage_z_plane()
    stage_mid(4)
    stage_last(2)
    stage_last(3)

    for b in range(2):
        total[:, b * AHEAD : (b + 1) * AHEAD] = mid_total(4, b)[0]
    for b in range(2):
        last = branches[b][9]
        result = total[:, b * AHEAD : (b + 1) * AHEAD]
        for k in range(7):
            last_copy(k, b).wait_recv()
            result = result + last[k].astype(F32)
        total[:, b * AHEAD : (b + 1) * AHEAD] = result
    result = gz[7, x, y].astype(F32)
    for n, copy in enumerate(plane_z_out):
        copy.wait_recv()
        result = result + plane_z[n + 1].astype(F32)
    total[:, 2 * AHEAD :] = result
    total_out = remote(
        total.at[pl.ds(pl.multiple_of(other * 8, 8), 8)],
        total_peer,
        total_sem.at[0],
        total_sem.at[1],
        **{C: other},
    )
    total_out.start()

    vec_c_out.wait_recv()
    grad_head_ref[:, half] = vec_c[0, :, :HALF]
    grad_head_ref[:, other_half] = vec_c[1, :, :HALF]
    loss_ref[...] = (vec_c[0, :, HALF:] + vec_c[1, :, HALF:]) * (1.0 / (STATES * 8))
    grad_ref[:, half] = total[pl.ds(pl.multiple_of(c * 8, 8), 8), :]

    sent = [pair, scores_out, vec_c_out]
    sent += state_out + lse_out + vec_x_out + vec_y_out + vec_z_out
    sent += far_z_out + plane_z_out
    sent += [rows_out(i) for i in range(3)]
    sent += [near_z_copy(j, s, h) for j in range(1, 4) for s in range(2) for h in range(2)]
    for copy in sent:
        copy.wait_send()

    for b in range(2):
        for n in range(len(GROUPS)):
            for copy in far_copies(n, b) + near_copies(n, b) + mid_copies(n, b):
                copy.wait_send()
        for k in range(7):
            last_copy(k, b).wait_send()
    total_out.wait()
    grad_ref[:, other_half] = total_peer[...]


def deliver(grad_in, grad_head_in, lse_in, loss_in, grad_out, grad_head_out, lse_out, loss_out):
    grad_out[...] = grad_in[...]
    grad_head_out[...] = grad_head_in[...]
    lse_out[...] = lse_in[...]
    loss_out[...] = loss_in[:, :1]


def body(state_features, action_features, targets, w_hidden, w_head):
    vmem = pl.BlockSpec(memory_space=pltpu.VMEM)
    anywhere = pl.BlockSpec(memory_space=pl.ANY)
    dma = pltpu.SemaphoreType.DMA
    scratch = [
        pltpu.VMEM((WIDTH, HALF), BF16),
        pltpu.VMEM((ROWS, WIDTH), BF16),
        pltpu.VMEM((64, 128), BF16),
        pltpu.VMEM((2, 16, 64, 128), BF16),
        pltpu.VMEM((STATES, WIDTH), F32),
        pltpu.VMEM((2 * ROWS, WIDTH), BF16),
        pltpu.VMEM((CHUNK, HALF), F32),
        pltpu.VMEM((CHUNK, HALF), F32),
        pltpu.VMEM((2 * ROWS, HALF), F32),
        pltpu.VMEM((2 * ROWS, HALF), F32),
        pltpu.VMEM((2 * ROWS, HALF), BF16),
        pltpu.VMEM((2 * ROWS, 128), F32),
        pltpu.VMEM((STATES, 128), F32),
        pltpu.VMEM((STATES, 128), F32),
        pltpu.VMEM((STATES, 128), F32),
        pltpu.VMEM((2 * ROWS, 128), F32),
        pltpu.VMEM((16, 1, 128), F32),
        pltpu.VMEM((4, 1, VECTOR), F32),
        pltpu.VMEM((4, 1, VECTOR), F32),
        pltpu.VMEM((8, 1, VECTOR), F32),
        pltpu.VMEM((2, 1, VECTOR), F32),
        pltpu.VMEM((len(GROUPS), 4, 4, DEPTH, 16, AHEAD), BF16),
        pltpu.VMEM((len(GROUPS), 4, 4, DEPTH, 16, AHEAD), BF16),
        pltpu.VMEM((8, 4, 4, 16, LAST), BF16),
        pltpu.VMEM((len(GROUPS), 2, 2, DEPTH, 16, AHEAD), BF16),
        pltpu.VMEM((len(GROUPS), 2, 2, DEPTH, 16, AHEAD), BF16),
        pltpu.VMEM((len(GROUPS), 2, 4, DEPTH, 16, AHEAD), BF16),
        pltpu.VMEM((len(GROUPS), 2, 4, DEPTH, 16, AHEAD), BF16),
        pltpu.VMEM((len(GROUPS), 3, DEPTH, 16, AHEAD), BF16),
        pltpu.VMEM((len(GROUPS), 3, DEPTH, 16, AHEAD), BF16),
        pltpu.VMEM((8, 16, AHEAD), BF16),
        pltpu.VMEM((8, 16, AHEAD), BF16),
        pltpu.VMEM((2, 2, 4, 16, LAST), BF16),
        pltpu.VMEM((2, 3, 4, 4, 16, LAST), BF16),
        pltpu.VMEM((16, 16, LAST), BF16),
        pltpu.VMEM((16, HALF), F32),
        pltpu.VMEM((8, HALF), F32),
        dma((4,)),
        dma((2,)),
        dma((2, 16)),
        dma((2, 3)),
        dma((2,)),
        dma((2, 16)),
        dma((2, 4)),
        dma((2, 4)),
        dma((2, 8)),
        dma((2,)),
        dma((2, 2, len(GROUPS), 2)),
        dma((2, 2, len(GROUPS), 2)),
        dma((2, 2, len(GROUPS), 3)),
        dma((2, 2, 8)),
        dma((2, 2)),
        dma((2, 2, 3, 2)),
        dma((2, 16)),
        dma((2,)),
    ]
    grad, grad_head, lse, loss = pl.pallas_call(
        kernel,
        out_shape=(
            jax.ShapeDtypeStruct((8, WIDTH), F32),
            jax.ShapeDtypeStruct((1, WIDTH), F32),
            jax.ShapeDtypeStruct((1, STATES), F32),
            jax.ShapeDtypeStruct((1, 128), F32),
        ),
        in_specs=[vmem, anywhere, vmem, anywhere, vmem],
        out_specs=(vmem,) * 4,
        scratch_shapes=scratch,
        compiler_params=pltpu.CompilerParams(
            collective_id=0, has_side_effects=True, vmem_limit_bytes=62 * 1024 * 1024
        ),
        name="critic",
    )(
        state_features.T,
        action_features.reshape(ROWS, WIDTH),
        targets.reshape(1, STATES),
        w_hidden,
        w_head.reshape(1, WIDTH),
    )
    grad, grad_head, lse, loss = pl.pallas_call(
        deliver,
        out_shape=(
            jax.ShapeDtypeStruct((8, WIDTH), F32),
            jax.ShapeDtypeStruct((1, WIDTH), F32),
            jax.ShapeDtypeStruct((1, STATES), F32),
            jax.ShapeDtypeStruct((1, 1), F32),
        ),
        in_specs=[vmem] * 4,
        out_specs=(vmem,) * 4,
        name="deliver",
    )(grad, grad_head, lse, loss)
    return grad, grad_head.reshape(WIDTH), lse.reshape(STATES), loss.reshape(())


def solution(mesh):
    finer = Mesh(mesh.devices.reshape(8, 4, 4, 2), (Z, X, Y, C))
    return jax.shard_map(
        body,
        mesh=finer,
        in_specs=(P(Z, ACT), P(Z, ACT, None), P(Z), P(), P()),
        out_specs=(P(STATE_ACT, None), P(), P(Z), P()),
        check_vma=False,
    )
```

```python
import jax
import jax.numpy as jnp
from jax import lax
from jax.experimental import pallas as pl
from jax.experimental.pallas import tpu as pltpu
from jax.sharding import Mesh
from jax.sharding import PartitionSpec as P

Z, X, Y, C = "state", "act_0", "act_1", "act_2"
ACT = (X, Y, C)
STATE_ACT = (Z, X, Y, C)

norm_epsilon = 1e-06
penalty_weight = 2.0

F32 = jnp.float32
BF16 = jnp.bfloat16
STATES = 96
ACTIONS = 8
ROWS = STATES * ACTIONS
WIDTH = 2048
HALF = WIDTH // 2
CHUNK = 256
SUB = 32
AHEAD = 384
LAST = 256
VECTOR = HALF + 128
GROUPS = ((0,), (1, 2), (3, 4), (5, 6), (7,))
DEPTH = 2
PLUS = {4: 0, 3: 1, 2: 3, 1: 5}
MINUS = {3: 2, 2: 4, 1: 6}


def remote(src, dst, send, recv, **target):
    return pltpu.make_async_remote_copy(
        src_ref=src,
        dst_ref=dst,
        send_sem=send,
        recv_sem=recv,
        device_id=target,
        device_id_type=pl.DeviceIdType.MESH,
    )


def take(ref, sem):
    pltpu.make_async_copy(ref, ref, sem).wait()


def kernel(
    state_ref,
    act_hbm,
    targets_ref,
    w_hbm,
    head_ref,
    grad_ref,
    grad_head_ref,
    lse_ref,
    loss_ref,
    w_buf,
    act_buf,
    state_own,
    state_all,
    state_f32,
    normed,
    state_pre,
    scale,
    head_in,
    slope,
    back,
    score_lanes,
    score_part,
    score_peer,
    score_grad,
    grad_rows,
    lse_all,
    vec_x,
    vec_y,
    vec_z,
    vec_c,
    gx,
    gy,
    gz,
    far_x,
    far_y,
    near_x,
    near_y,
    mid_x,
    mid_y,
    last_x,
    last_y,
    far_z,
    near_z,
    plane_z,
    total,
    total_peer,
    sem_in,
    pair_sem,
    state_sem,
    acts_sem,
    rows_sem,
    scale_sem,
    score_sem,
    lse_sem,
    vec_x_sem,
    vec_y_sem,
    vec_z_sem,
    vec_c_sem,
    far_sem,
    near_sem,
    mid_sem,
    last_sem,
    far_z_sem,
    near_z_sem,
    plane_z_sem,
    total_sem,
):
    z, x, y, c = (lax.axis_index(name) for name in (Z, X, Y, C))
    other = 1 - c
    half = pl.ds(pl.multiple_of(c * HALF, HALF), HALF)
    other_half = pl.ds(pl.multiple_of(other * HALF, HALF), HALF)

    def at(axis, step):
        if axis == Z:
            return lax.rem(z + step + 8, 8)
        return lax.rem((x if axis == X else y) + step + 4, 4)

    act_in = [
        pltpu.make_async_copy(
            act_hbm.at[pl.ds(i * CHUNK, CHUNK)], act_buf.at[pl.ds(i * CHUNK, CHUNK)], sem_in.at[i]
        )
        for i in range(3)
    ]
    w_in = pltpu.make_async_copy(w_hbm.at[:, half], w_buf, sem_in.at[3])
    for copy in act_in:
        copy.start()
    w_in.start()

    barrier = pltpu.get_barrier_semaphore()
    plane = [(dx, dy) for dx in range(4) for dy in range(4) if dx or dy]

    def greet(**target):
        pl.semaphore_signal(barrier, inc=1, device_id=target, device_id_type=pl.DeviceIdType.MESH)

    greet(**{C: other})
    for dx, dy in plane:
        greet(**{X: at(X, dx), Y: at(Y, dy)})
    for dz in range(1, 8):
        greet(**{Z: at(Z, dz)})
    pl.semaphore_wait(barrier, 1 + len(plane) + 7)

    state_own[...] = jnp.zeros(state_own.shape, BF16)
    state_own[:, :STATES] = state_ref[...]
    state_all[c, 0] = state_own[...]
    state_out = [
        remote(
            state_own,
            state_all.at[c, dx * 4 + dy],
            state_sem.at[0],
            state_sem.at[1],
            **{X: at(X, dx), Y: at(Y, dy)},
        )
        for dx, dy in plane
    ]
    for copy in state_out:
        copy.start()

    def shared(ref, sem, i):
        return remote(
            ref.at[pl.ds(i * CHUNK, CHUNK)],
            ref.at[pl.ds(ROWS + i * CHUNK, CHUNK)],
            sem.at[0],
            sem.at[1 + i],
            **{C: other},
        )

    acts_out = [shared(act_buf, acts_sem, i) for i in range(3)]
    for i in range(3):
        act_in[i].wait()
        acts_out[i].start()
    w_in.wait()
    for i in range(6):
        if i >= 3:
            acts_out[i - 3].wait_recv()
        rows = slice(i * CHUNK, (i + 1) * CHUNK)
        head_in[rows, :] = jnp.dot(act_buf[rows, :], w_buf[...], preferred_element_type=F32)

    take(state_all.at[0, pl.ds(0, 15)], state_sem.at[1])
    pair = remote(state_all.at[c], state_all.at[c], pair_sem.at[0], pair_sem.at[1], **{C: other})
    pair_in = remote(
        state_all.at[other], state_all.at[other], pair_sem.at[0], pair_sem.at[1], **{C: other}
    )
    pair.start()
    pair_in.wait_recv()
    for j in range(16):
        slot = lax.rem(x - j // 4 + 4, 4) * 4 + lax.rem(y - j % 4 + 4, 4)
        tile = jnp.concatenate([state_all[0, slot], state_all[1, slot]], 0).astype(F32)
        state_f32[:, j * 128 : (j + 1) * 128] = tile.T[:STATES, :]

    state_pre[...] = jnp.dot(
        state_f32[...].astype(BF16), w_buf[...], preferred_element_type=F32
    )

    rows_out = [shared(normed, rows_sem, i) for i in range(3)]
    scale_out = [shared(scale, scale_sem, i) for i in range(3)]

    def mixture(u, j):
        tile = slice(j * 128, (j + 1) * 128)
        lines = state_f32[u * 8 : u * 8 + 8, tile]
        lines = jnp.broadcast_to(lines[:, None, :], (8, 8, 128)).reshape(64, 128)
        return lines + act_buf[u * 64 : u * 64 + 64, tile].astype(F32)

    def normalise(i):
        for u in range(i * 4, i * 4 + 4):
            rows = slice(u * 64, u * 64 + 64)
            sums = None
            for j in range(WIDTH // 128):
                m = mixture(u, j)
                sums = m * m if sums is None else sums + m * m
            mean = jnp.sum(sums, -1, keepdims=True) * (1.0 / WIDTH)
            factor = jnp.broadcast_to(lax.rsqrt(mean + norm_epsilon), (64, 128))
            scale[rows, :] = factor
            for j in range(WIDTH // 128):
                normed[rows, j * 128 : (j + 1) * 128] = (mixture(u, j) * factor).astype(BF16)

    lane8 = lax.broadcasted_iota(jnp.int32, (8, 128), 1)
    row8 = lax.broadcasted_iota(jnp.int32, (8, 128), 0)

    def finish(i):
        w = head_ref[:, half]
        for t in range(CHUNK // SUB):
            rows = slice(i * CHUNK + t * SUB, i * CHUNK + (t + 1) * SUB)
            state = (i % 3) * (CHUNK // 8) + t * (SUB // 8)
            line = state_pre[state : state + SUB // 8, :]
            line = jnp.broadcast_to(line[:, None, :], (SUB // 8, 8, HALF)).reshape(SUB, HALF)
            factor = jnp.concatenate([scale[rows, :]] * (HALF // 128), 1)
            p = factor * (head_in[rows, :] + line)
            g = 0.5 * jnp.tanh(0.5 * p) + 0.5
            pg = p * g
            h = normed[rows, half].astype(F32) + pg
            head_in[rows, :] = h
            slope[rows, :] = w * (g + pg * (1.0 - g))
            hw = h * w
            sums = hw[:, :128]
            for j in range(1, HALF // 128):
                sums = sums + hw[:, j * 128 : (j + 1) * 128]
            score_lanes[rows, :] = sums

    for i in range(3):
        normalise(i)
        rows_out[i].start()
        scale_out[i].start()
    for i in range(6):
        if i >= 3:
            rows_out[i - 3].wait_recv()
            scale_out[i - 3].wait_recv()
        finish(i)

    for i in range(3):
        states = 0.0
        for part, core in ((0, c), (1, other)):
            first = part * ROWS + i * CHUNK
            column = jnp.sum(score_lanes[first : first + CHUNK, :], -1, keepdims=True)
            column = column.reshape(CHUNK // 8, 8, 1)
            states = states + jnp.sum(
                jnp.where((lane8 == row8 + core * 8)[None], column, 0.0), 1
            )
        score_part[i * (CHUNK // 8) : (i + 1) * (CHUNK // 8), :] = states
    scores_out = remote(score_part, score_peer, score_sem.at[0], score_sem.at[1], **{C: other})
    scores_out.start()
    scores_out.wait_recv()
    scores = score_part[...] + score_peer[...]
    lane = lax.broadcasted_iota(jnp.int32, (STATES, 128), 1)
    row = lax.broadcasted_iota(jnp.int32, (STATES, 128), 0)
    valid = lane < 16
    eye = lane == row
    top = jnp.max(jnp.where(valid, scores, -jnp.inf), -1, keepdims=True)
    local = jnp.sum(jnp.where(valid, jnp.exp(scores - top), 0.0), -1, keepdims=True)
    lse_all[0] = jnp.sum(jnp.where(eye, top + jnp.log(local), 0.0), 0, keepdims=True)
    lse_out = [
        remote(
            lse_all.at[0],
            lse_all.at[dx * 4 + dy],
            lse_sem.at[0],
            lse_sem.at[1],
            **{X: at(X, dx), Y: at(Y, dy)},
        )
        for dx, dy in plane
    ]
    for copy in lse_out:
        copy.start()
    take(lse_all.at[pl.ds(0, 15)], lse_sem.at[1])
    parts = [
        lse_all[lax.rem(x - j // 4 + 4, 4) * 4 + lax.rem(y - j % 4 + 4, 4)] for j in range(16)
    ]
    peak = parts[0]
    for part in parts[1:]:
        peak = jnp.maximum(peak, part)
    mass = jnp.exp(parts[0] - peak)
    for part in parts[1:]:
        mass = mass + jnp.exp(part - peak)
    lse_row = peak + jnp.log(mass)
    lse_ref[...] = lse_row[:, :STATES]
    lse = jnp.sum(jnp.where(eye, lse_row, 0.0), -1, keepdims=True)
    eye_states = lax.broadcasted_iota(jnp.int32, (STATES, STATES), 1) == lax.broadcasted_iota(
        jnp.int32, (STATES, STATES), 0
    )
    target = jnp.sum(jnp.where(eye_states, targets_ref[...], 0.0), -1, keepdims=True)
    data_lane = jnp.where((x == 0) & (y == 0), 0, -1)
    is_data = lane == data_lane
    gap = scores - target
    score_grad[...] = jnp.where(
        valid, penalty_weight * jnp.exp(scores - lse), 0.0
    ) + jnp.where(is_data, gap - penalty_weight, 0.0)
    loss_terms = jnp.where(is_data, penalty_weight * (lse - scores) + 0.5 * gap * gap, 0.0)
    loss_here = jnp.sum(jnp.sum(loss_terms, 0, keepdims=True), -1, keepdims=True)
    loss_here = jnp.where(c == 0, loss_here, 0.0)

    for part, core in ((0, c), (1, other)):
        for i in range(3):
            lines = score_grad[i * (CHUNK // 8) : (i + 1) * (CHUNK // 8), :]
            lines = jnp.broadcast_to(lines[:, None, :], (CHUNK // 8, 8, 128))
            lines = jnp.where((lane8 == row8 + core * 8)[None], lines, 0.0)
            column = jnp.sum(lines.reshape(CHUNK, 128), -1, keepdims=True)
            first = part * ROWS + i * CHUNK
            grad_rows[first : first + CHUNK, :] = jnp.broadcast_to(column, (CHUNK, 128))

    def backward(t, head_sum):
        rows = pl.ds(pl.multiple_of(t * SUB, SUB), SUB)
        g = jnp.concatenate([grad_rows[rows, :]] * (HALF // 128), 1)
        back[rows, :] = (g * slope[rows, :]).astype(BF16)
        return head_sum + jnp.sum((g * head_in[rows, :]).reshape(SUB // 8, 8, HALF), 0)

    head_sum = lax.fori_loop(0, 2 * ROWS // SUB, backward, jnp.zeros((8, HALF), F32), unroll=2)
    vec_x[0, :, :HALF] = jnp.sum(head_sum, 0, keepdims=True)
    vec_x[0, :, HALF:] = jnp.broadcast_to(loss_here, (1, 128))

    def vec_copies(axis, buf, sem, count):
        return [
            remote(buf.at[0], buf.at[d], sem.at[0], sem.at[1], **{axis: at(axis, d)})
            for d in range(1, count)
        ]

    def vec_sum(buf, me, count):
        result = buf[me]
        for q in range(1, count):
            result = result + buf[lax.rem(me - q + count, count)]
        return result

    vec_x_out = vec_copies(X, vec_x, vec_x_sem, 4)
    vec_y_out = vec_copies(Y, vec_y, vec_y_sem, 4)
    vec_z_out = vec_copies(Z, vec_z, vec_z_sem, 8)
    vec_c_out = remote(vec_c.at[0], vec_c.at[1], vec_c_sem.at[0], vec_c_sem.at[1], **{C: other})
    for copy in vec_x_out:
        copy.start()

    def vec_step_y():
        take(vec_x.at[pl.ds(0, 3)], vec_x_sem.at[1])
        vec_y[0] = vec_sum(vec_x, x, 4)
        for copy in vec_y_out:
            copy.start()

    def vec_step_z():
        take(vec_y.at[pl.ds(0, 3)], vec_y_sem.at[1])
        vec_z[0] = vec_sum(vec_y, y, 4)
        for copy in vec_z_out:
            copy.start()

    def vec_step_c():
        take(vec_z.at[pl.ds(0, 7)], vec_z_sem.at[1])
        vec_c[0] = vec_sum(vec_z, z, 8)
        vec_c_out.start()

    def target_z(k):
        return lax.rem(z + jnp.where(lax.rem(k, 2) == 1, 4 - (k + 1) // 2, 4 + k // 2), 8)

    branches = (
        (0, X, Y, x, y, gx, far_x, near_x, mid_x, last_x),
        (1, Y, X, y, x, gy, far_y, near_y, mid_y, last_y),
    )

    def held(n):
        return pl.ds(0, len(GROUPS[n]))

    def far_copies(n, b):
        i, axis, _, me, _, g, far, _, _, _ = branches[b]
        return [
            remote(
                g.at[n, at(axis, 2), pl.ds(2 * s, 2), held(n)],
                far.at[n, s, :, held(n)],
                far_sem.at[i, 0],
                far_sem.at[i, 1 + 2 * n + s],
                **{axis: at(axis, 1 - 2 * s)},
            )
            for s in range(2)
        ]

    def near_copies(n, b):
        i, axis, _, me, _, g, _, near, _, _ = branches[b]
        return [
            remote(
                g.at[n, at(axis, 1 - 2 * s), :, held(n)],
                near.at[n, s, :, held(n)],
                near_sem.at[i, 0],
                near_sem.at[i, 1 + n],
                **{axis: at(axis, 1 - 2 * s)},
            )
            for s in range(2)
        ]

    def mid_copies(n, b):
        i, _, axis, me, _, g, _, _, mid, _ = branches[b]
        return [
            remote(
                g.at[n, me, at(axis, d), held(n)],
                mid.at[n, d - 1, held(n)],
                mid_sem.at[i, 0],
                mid_sem.at[i, 1 + n],
                **{axis: at(axis, d)},
            )
            for d in range(1, 4)
        ]

    def last_copy(k, b):
        i, _, _, me, me2, g, _, _, _, last = branches[b]
        return remote(
            g.at[(k + 1) // 2, me, me2, 0 if k == 0 else (k + 1) % 2],
            last.at[k],
            last_sem.at[i, 0],
            last_sem.at[i, 1],
            **{Z: target_z(k)},
        )

    def block(n, d):
        k = GROUPS[n][0] + d
        columns = pl.ds(pl.multiple_of(target_z(k) * 256, 256), 256)
        result = lax.dot_general(
            normed[:, columns],
            back[...],
            (((0,), (0,)), ((), ())),
            preferred_element_type=F32,
        ).astype(BF16)
        for i in range(4):
            for j in range(4):
                part = result[i * 64 + j * 16 : i * 64 + j * 16 + 16, :]
                gx[n, i, j, d] = part[:, :AHEAD]
                gy[n, j, i, d] = part[:, AHEAD : 2 * AHEAD]
                gz[k, i, j] = part[:, 2 * AHEAD :]

    def stage_block(n):
        def one(d, carry):
            block(n, d)
            return carry

        lax.fori_loop(0, len(GROUPS[n]), one, 0)
        for b in range(2):
            for copy in far_copies(n, b):
                copy.start()

    def stage_near(n):
        for b in range(2):
            _, axis, _, _, _, g, far, _, _, _ = branches[b]
            copies = near_copies(n, b)
            for s, arrived in enumerate(far_copies(n, b)):
                arrived.wait_recv()
                ref = g.at[n, at(axis, 1 - 2 * s), pl.ds(2 * s, 2), held(n)]
                ref[...] = (
                    ref[...].astype(F32) + far[n, s, :, held(n)].astype(F32)
                ).astype(BF16)
                copies[s].start()

    def stage_mid(n):
        for b in range(2):
            _, _, _, me, _, g, _, near, _, _ = branches[b]
            take(near.at[n, :, :, held(n)], near_sem.at[b, 1 + n])
            ref = g.at[n, me, :, held(n)]
            ref[...] = (
                ref[...].astype(F32)
                + near[n, 0, :, held(n)].astype(F32)
                + near[n, 1, :, held(n)].astype(F32)
            ).astype(BF16)
            for copy in mid_copies(n, b):
                copy.start()

    def mid_total(n, b):
        _, _, _, me, me2, g, _, _, mid, _ = branches[b]
        take(mid.at[n, :, held(n)], mid_sem.at[b, 1 + n])
        result = g[n, me, me2, held(n)].astype(F32)
        for d in range(3):
            result = result + mid[n, d, held(n)].astype(F32)
        return result

    def stage_last(n):
        for b in range(2):
            _, _, _, me, me2, g, _, _, _, _ = branches[b]
            g[n, me, me2, held(n)] = mid_total(n, b).astype(BF16)
            for k in GROUPS[n]:
                last_copy(k, b).start()

    far_z_out = [
        remote(
            gz.at[PLUS[4], pl.ds(2 * s, 2)],
            far_z.at[s],
            far_z_sem.at[0],
            far_z_sem.at[1 + s],
            **{Z: at(Z, 1 - 2 * s)},
        )
        for s in range(2)
    ]

    def near_z_copy(j, s, h):
        return remote(
            gz.at[(PLUS, MINUS)[s][j], pl.ds(2 * h, 2)],
            near_z.at[s, j - 1, pl.ds(2 * h, 2)],
            near_z_sem.at[0],
            near_z_sem.at[1 + s * 6 + (j - 1) * 2 + h],
            **{Z: at(Z, 1 - 2 * s)},
        )

    def stage_z(j, late):
        for s in range(2):
            h = s if late else 1 - s
            ref = gz.at[(PLUS, MINUS)[s][j], pl.ds(2 * h, 2)]
            arrived = None
            if j < 3:
                near_z_copy(j + 1, s, h).wait_recv()
                arrived = near_z[s, j, pl.ds(2 * h, 2)]
            elif late:
                far_z_out[s].wait_recv()
                arrived = far_z[s]
            if arrived is not None:
                ref[...] = (ref[...].astype(F32) + arrived.astype(F32)).astype(BF16)
            near_z_copy(j, s, h).start()

    plane_z_out = [
        remote(
            gz.at[7, at(X, dx), at(Y, dy)],
            plane_z.at[dx * 4 + dy],
            plane_z_sem.at[0],
            plane_z_sem.at[1],
            **{X: at(X, dx), Y: at(Y, dy)},
        )
        for dx, dy in plane
    ]

    def stage_z_plane():
        for s in range(2):
            for h in range(2):
                near_z_copy(1, s, h).wait_recv()
        gz[7] = (
            gz[7].astype(F32) + near_z[0, 0].astype(F32) + near_z[1, 0].astype(F32)
        ).astype(BF16)
        for copy in plane_z_out:
            copy.start()

    stage_block(0)
    for copy in far_z_out:
        copy.start()
    stage_block(1)
    stage_z(3, 0)
    stage_block(2)
    vec_step_y()
    stage_near(0)
    stage_z(3, 1)
    stage_block(3)
    stage_block(4)
    stage_near(1)
    stage_z(2, 0)
    stage_near(2)
    stage_z(2, 1)
    stage_mid(0)
    vec_step_z()
    stage_near(3)
    stage_near(4)
    stage_z(1, 0)
    stage_mid(1)
    stage_z(1, 1)
    stage_mid(2)
    stage_last(0)
    vec_step_c()
    stage_mid(3)
    stage_z_plane()
    stage_mid(4)
    stage_last(1)
    stage_last(2)
    stage_last(3)

    for b in range(2):
        total[:, b * AHEAD : (b + 1) * AHEAD] = mid_total(4, b)[0]
    for b in range(2):
        last = branches[b][9]
        result = total[:, b * AHEAD : (b + 1) * AHEAD]
        take(last.at[pl.ds(0, 7)], last_sem.at[b, 1])
        for k in range(7):
            result = result + last[k].astype(F32)
        total[:, b * AHEAD : (b + 1) * AHEAD] = result
    result = gz[7, x, y].astype(F32)
    take(plane_z.at[pl.ds(0, 15)], plane_z_sem.at[1])
    for n in range(1, 16):
        result = result + plane_z[n].astype(F32)
    total[:, 2 * AHEAD :] = result
    total_out = remote(
        total.at[pl.ds(pl.multiple_of(other * 8, 8), 8)],
        total_peer,
        total_sem.at[0],
        total_sem.at[1],
        **{C: other},
    )
    total_out.start()

    vec_c_out.wait_recv()
    grad_head_ref[:, half] = vec_c[0, :, :HALF]
    grad_head_ref[:, other_half] = vec_c[1, :, :HALF]
    loss_ref[...] = (vec_c[0, :, HALF:] + vec_c[1, :, HALF:]) * (1.0 / (STATES * 8))
    grad_ref[:, half] = total[pl.ds(pl.multiple_of(c * 8, 8), 8), :]

    for copy in (pair, scores_out, vec_c_out):
        copy.wait_send()
    for ref, sem in (
        (state_all.at[0, pl.ds(0, 15)], state_sem),
        (lse_all.at[pl.ds(0, 15)], lse_sem),
        (act_buf.at[pl.ds(0, ROWS)], acts_sem),
        (normed.at[pl.ds(0, ROWS)], rows_sem),
        (scale.at[pl.ds(0, ROWS)], scale_sem),
        (vec_x.at[pl.ds(0, 3)], vec_x_sem),
        (vec_y.at[pl.ds(0, 3)], vec_y_sem),
        (vec_z.at[pl.ds(0, 7)], vec_z_sem),
        (gz.at[0], far_z_sem),
        (gz.at[pl.ds(0, 6)], near_z_sem),
        (plane_z.at[pl.ds(0, 15)], plane_z_sem),
    ):
        take(ref, sem.at[0])
    for b in range(2):
        take(gx.at[0], far_sem.at[b, 0])
        take(gx.at[pl.ds(0, 2)], near_sem.at[b, 0])
        take(gx.at[0, pl.ds(0, 3)], mid_sem.at[b, 0])
        take(last_x.at[pl.ds(0, 7)], last_sem.at[b, 0])
    total_out.wait()
    grad_ref[:, other_half] = total_peer[...]


def deliver(grad_in, grad_head_in, lse_in, loss_in, grad_out, grad_head_out, lse_out, loss_out):
    grad_out[...] = grad_in[...]
    grad_head_out[...] = grad_head_in[...]
    lse_out[...] = lse_in[...]
    loss_out[...] = loss_in[:, :1]


def body(state_features, action_features, targets, w_hidden, w_head):
    vmem = pl.BlockSpec(memory_space=pltpu.VMEM)
    anywhere = pl.BlockSpec(memory_space=pl.ANY)
    dma = pltpu.SemaphoreType.DMA
    scratch = [
        pltpu.VMEM((WIDTH, HALF), BF16),
        pltpu.VMEM((2 * ROWS, WIDTH), BF16),
        pltpu.VMEM((64, 128), BF16),
        pltpu.VMEM((2, 16, 64, 128), BF16),
        pltpu.VMEM((STATES, WIDTH), F32),
        pltpu.VMEM((2 * ROWS, WIDTH), BF16),
        pltpu.VMEM((STATES, HALF), F32),
        pltpu.VMEM((2 * ROWS, 128), F32),
        pltpu.VMEM((2 * ROWS, HALF), F32),
        pltpu.VMEM((2 * ROWS, HALF), F32),
        pltpu.VMEM((2 * ROWS, HALF), BF16),
        pltpu.VMEM((2 * ROWS, 128), F32),
        pltpu.VMEM((STATES, 128), F32),
        pltpu.VMEM((STATES, 128), F32),
        pltpu.VMEM((STATES, 128), F32),
        pltpu.VMEM((2 * ROWS, 128), F32),
        pltpu.VMEM((16, 1, 128), F32),
        pltpu.VMEM((4, 1, VECTOR), F32),
        pltpu.VMEM((4, 1, VECTOR), F32),
        pltpu.VMEM((8, 1, VECTOR), F32),
        pltpu.VMEM((2, 1, VECTOR), F32),
        pltpu.VMEM((len(GROUPS), 4, 4, DEPTH, 16, AHEAD), BF16),
        pltpu.VMEM((len(GROUPS), 4, 4, DEPTH, 16, AHEAD), BF16),
        pltpu.VMEM((8, 4, 4, 16, LAST), BF16),
        pltpu.VMEM((len(GROUPS), 2, 2, DEPTH, 16, AHEAD), BF16),
        pltpu.VMEM((len(GROUPS), 2, 2, DEPTH, 16, AHEAD), BF16),
        pltpu.VMEM((len(GROUPS), 2, 4, DEPTH, 16, AHEAD), BF16),
        pltpu.VMEM((len(GROUPS), 2, 4, DEPTH, 16, AHEAD), BF16),
        pltpu.VMEM((len(GROUPS), 3, DEPTH, 16, AHEAD), BF16),
        pltpu.VMEM((len(GROUPS), 3, DEPTH, 16, AHEAD), BF16),
        pltpu.VMEM((8, 16, AHEAD), BF16),
        pltpu.VMEM((8, 16, AHEAD), BF16),
        pltpu.VMEM((2, 2, 4, 16, LAST), BF16),
        pltpu.VMEM((2, 3, 4, 4, 16, LAST), BF16),
        pltpu.VMEM((16, 16, LAST), BF16),
        pltpu.VMEM((16, HALF), F32),
        pltpu.VMEM((8, HALF), F32),
        dma((4,)),
        dma((2,)),
        dma((2,)),
        dma((4,)),
        dma((4,)),
        dma((4,)),
        dma((2,)),
        dma((2,)),
        dma((2,)),
        dma((2,)),
        dma((2,)),
        dma((2,)),
        dma((2, 1 + 2 * len(GROUPS))),
        dma((2, 1 + len(GROUPS))),
        dma((2, 1 + len(GROUPS))),
        dma((2, 2)),
        dma((3,)),
        dma((13,)),
        dma((2,)),
        dma((2,)),
    ]
    grad, grad_head, lse, loss = pl.pallas_call(
        kernel,
        out_shape=(
            jax.ShapeDtypeStruct((8, WIDTH), F32),
            jax.ShapeDtypeStruct((1, WIDTH), F32),
            jax.ShapeDtypeStruct((1, STATES), F32),
            jax.ShapeDtypeStruct((1, 128), F32),
        ),
        in_specs=[vmem, anywhere, vmem, anywhere, vmem],
        out_specs=(vmem,) * 4,
        scratch_shapes=scratch,
        compiler_params=pltpu.CompilerParams(
            collective_id=0, has_side_effects=True, vmem_limit_bytes=62 * 1024 * 1024
        ),
        name="critic",
    )(
        state_features.T,
        action_features.reshape(ROWS, WIDTH),
        targets.reshape(1, STATES),
        w_hidden,
        w_head.reshape(1, WIDTH),
    )
    grad, grad_head, lse, loss = pl.pallas_call(
        deliver,
        out_shape=(
            jax.ShapeDtypeStruct((8, WIDTH), F32),
            jax.ShapeDtypeStruct((1, WIDTH), F32),
            jax.ShapeDtypeStruct((1, STATES), F32),
            jax.ShapeDtypeStruct((1, 1), F32),
        ),
        in_specs=[vmem] * 4,
        out_specs=(vmem,) * 4,
        name="deliver",
    )(grad, grad_head, lse, loss)
    return grad, grad_head.reshape(WIDTH), lse.reshape(STATES), loss.reshape(())


def solution(mesh):
    finer = Mesh(mesh.devices.reshape(8, 4, 4, 2), (Z, X, Y, C))
    return jax.shard_map(
        body,
        mesh=finer,
        in_specs=(P(Z, ACT), P(Z, ACT, None), P(Z), P(), P()),
        out_specs=(P(STATE_ACT, None), P(), P(Z), P()),
        check_vma=False,
    )
```

```python
import jax
import jax.numpy as jnp
from jax import lax
from jax.experimental import pallas as pl
from jax.experimental.pallas import tpu as pltpu
from jax.sharding import Mesh
from jax.sharding import PartitionSpec as P

Z, X, Y, C = "state", "act_0", "act_1", "act_2"
ACT = (X, Y, C)
STATE_ACT = (Z, X, Y, C)

norm_epsilon = 1e-06
penalty_weight = 2.0

F32 = jnp.float32
BF16 = jnp.bfloat16
STATES = 96
ACTIONS = 8
ROWS = STATES * ACTIONS
WIDTH = 2048
HALF = WIDTH // 2
CHUNK = 256
SUB = 32
AHEAD = 384
LAST = 256
VECTOR = HALF + 128
GROUPS = ((0,), (1, 2), (3, 4), (5, 6), (7,))
DEPTH = 2
PLUS = {4: 0, 3: 1, 2: 3, 1: 5}
MINUS = {3: 2, 2: 4, 1: 6}


def remote(src, dst, send, recv, **target):
    return pltpu.make_async_remote_copy(
        src_ref=src,
        dst_ref=dst,
        send_sem=send,
        recv_sem=recv,
        device_id=target,
        device_id_type=pl.DeviceIdType.MESH,
    )


def take(ref, sem):
    pltpu.make_async_copy(ref, ref, sem).wait()


def kernel(
    state_ref,
    act_hbm,
    targets_ref,
    w_hbm,
    head_ref,
    grad_ref,
    grad_head_ref,
    lse_ref,
    loss_ref,
    w_buf,
    act_buf,
    state_own,
    state_all,
    state_f32,
    normed,
    state_pre,
    scale,
    head_in,
    slope,
    back,
    score_lanes,
    score_part,
    score_peer,
    score_grad,
    grad_rows,
    lse_all,
    vec_x,
    vec_y,
    vec_z,
    vec_c,
    gx,
    gy,
    gz,
    far_x,
    far_y,
    near_x,
    near_y,
    mid_x,
    mid_y,
    last_x,
    last_y,
    far_z,
    near_z,
    plane_z,
    total,
    total_peer,
    sem_in,
    pair_sem,
    state_sem,
    acts_sem,
    rows_sem,
    scale_sem,
    score_sem,
    lse_sem,
    vec_x_sem,
    vec_y_sem,
    vec_z_sem,
    vec_c_sem,
    far_sem,
    near_sem,
    mid_sem,
    last_sem,
    far_z_sem,
    near_z_sem,
    plane_z_sem,
    total_sem,
):
    z, x, y, c = (lax.axis_index(name) for name in (Z, X, Y, C))
    other = 1 - c
    half = pl.ds(pl.multiple_of(c * HALF, HALF), HALF)
    other_half = pl.ds(pl.multiple_of(other * HALF, HALF), HALF)

    def at(axis, step):
        if axis == Z:
            return lax.rem(z + step + 8, 8)
        return lax.rem((x if axis == X else y) + step + 4, 4)

    act_in = [
        pltpu.make_async_copy(
            act_hbm.at[pl.ds(i * CHUNK, CHUNK)], act_buf.at[pl.ds(i * CHUNK, CHUNK)], sem_in.at[i]
        )
        for i in range(3)
    ]
    w_in = pltpu.make_async_copy(w_hbm.at[:, half], w_buf, sem_in.at[3])
    for copy in act_in:
        copy.start()
    w_in.start()

    barrier = pltpu.get_barrier_semaphore()
    plane = [(dx, dy) for dx in range(4) for dy in range(4) if dx or dy]

    def greet(**target):
        pl.semaphore_signal(barrier, inc=1, device_id=target, device_id_type=pl.DeviceIdType.MESH)

    greet(**{C: other})
    for dx, dy in plane:
        greet(**{X: at(X, dx), Y: at(Y, dy)})
    for dz in range(1, 8):
        greet(**{Z: at(Z, dz)})
    pl.semaphore_wait(barrier, 1 + len(plane) + 7)

    state_own[...] = jnp.zeros(state_own.shape, BF16)
    state_own[:, :STATES] = state_ref[...]
    state_all[c, 0] = state_own[...]
    state_out = [
        remote(
            state_own,
            state_all.at[c, dx * 4 + dy],
            state_sem.at[0],
            state_sem.at[1],
            **{X: at(X, dx), Y: at(Y, dy)},
        )
        for dx, dy in plane
    ]
    for copy in state_out:
        copy.start()

    def shared(ref, sem, i):
        return remote(
            ref.at[pl.ds(i * CHUNK, CHUNK)],
            ref.at[pl.ds(ROWS + i * CHUNK, CHUNK)],
            sem.at[0],
            sem.at[1 + i],
            **{C: other},
        )

    acts_out = [shared(act_buf, acts_sem, i) for i in range(3)]
    for i in range(3):
        act_in[i].wait()
        acts_out[i].start()
    w_in.wait()
    for i in range(6):
        if i >= 3:
            acts_out[i - 3].wait_recv()
        rows = slice(i * CHUNK, (i + 1) * CHUNK)
        head_in[rows, :] = jnp.dot(act_buf[rows, :], w_buf[...], preferred_element_type=F32)

    take(state_all.at[0, pl.ds(0, 15)], state_sem.at[1])
    pair = remote(state_all.at[c], state_all.at[c], pair_sem.at[0], pair_sem.at[1], **{C: other})
    pair_in = remote(
        state_all.at[other], state_all.at[other], pair_sem.at[0], pair_sem.at[1], **{C: other}
    )
    pair.start()
    pair_in.wait_recv()
    for j in range(16):
        slot = lax.rem(x - j // 4 + 4, 4) * 4 + lax.rem(y - j % 4 + 4, 4)
        tile = jnp.concatenate([state_all[0, slot], state_all[1, slot]], 0).astype(F32)
        state_f32[:, j * 128 : (j + 1) * 128] = tile.T[:STATES, :]

    state_pre[...] = jnp.dot(
        state_f32[...].astype(BF16), w_buf[...], preferred_element_type=F32
    )

    rows_out = [shared(normed, rows_sem, i) for i in range(3)]
    scale_out = [shared(scale, scale_sem, i) for i in range(3)]

    def mixture(u, j):
        tile = slice(j * 128, (j + 1) * 128)
        lines = state_f32[u * 8 : u * 8 + 8, tile]
        lines = jnp.broadcast_to(lines[:, None, :], (8, 8, 128)).reshape(64, 128)
        return lines + act_buf[u * 64 : u * 64 + 64, tile].astype(F32)

    def normalise(i):
        for u in range(i * 4, i * 4 + 4):
            rows = slice(u * 64, u * 64 + 64)
            sums = None
            for j in range(WIDTH // 128):
                m = mixture(u, j)
                sums = m * m if sums is None else sums + m * m
            mean = jnp.sum(sums, -1, keepdims=True) * (1.0 / WIDTH)
            factor = jnp.broadcast_to(lax.rsqrt(mean + norm_epsilon), (64, 128))
            scale[rows, :] = factor
            for j in range(WIDTH // 128):
                normed[rows, j * 128 : (j + 1) * 128] = (mixture(u, j) * factor).astype(BF16)

    lane8 = lax.broadcasted_iota(jnp.int32, (8, 128), 1)
    row8 = lax.broadcasted_iota(jnp.int32, (8, 128), 0)

    def finish(i):
        w = head_ref[:, half]
        for t in range(CHUNK // SUB):
            rows = slice(i * CHUNK + t * SUB, i * CHUNK + (t + 1) * SUB)
            state = (i % 3) * (CHUNK // 8) + t * (SUB // 8)
            line = state_pre[state : state + SUB // 8, :]
            line = jnp.broadcast_to(line[:, None, :], (SUB // 8, 8, HALF)).reshape(SUB, HALF)
            factor = jnp.concatenate([scale[rows, :]] * (HALF // 128), 1)
            p = factor * (head_in[rows, :] + line)
            g = 0.5 * jnp.tanh(0.5 * p) + 0.5
            pg = p * g
            h = normed[rows, half].astype(F32) + pg
            head_in[rows, :] = h
            slope[rows, :] = w * (g + pg * (1.0 - g))
            hw = h * w
            sums = hw[:, :128]
            for j in range(1, HALF // 128):
                sums = sums + hw[:, j * 128 : (j + 1) * 128]
            score_lanes[rows, :] = sums

    for i in range(3):
        normalise(i)
        rows_out[i].start()
        scale_out[i].start()
    for i in range(6):
        if i >= 3:
            rows_out[i - 3].wait_recv()
            scale_out[i - 3].wait_recv()
        finish(i)

    for i in range(3):
        states = 0.0
        for part, core in ((0, c), (1, other)):
            first = part * ROWS + i * CHUNK
            column = jnp.sum(score_lanes[first : first + CHUNK, :], -1, keepdims=True)
            column = column.reshape(CHUNK // 8, 8, 1)
            states = states + jnp.sum(
                jnp.where((lane8 == row8 + core * 8)[None], column, 0.0), 1
            )
        score_part[i * (CHUNK // 8) : (i + 1) * (CHUNK // 8), :] = states
    scores_out = remote(score_part, score_peer, score_sem.at[0], score_sem.at[1], **{C: other})
    scores_out.start()
    scores_out.wait_recv()
    scores = score_part[...] + score_peer[...]
    lane = lax.broadcasted_iota(jnp.int32, (STATES, 128), 1)
    row = lax.broadcasted_iota(jnp.int32, (STATES, 128), 0)
    valid = lane < 16
    eye = lane == row
    top = jnp.max(jnp.where(valid, scores, -jnp.inf), -1, keepdims=True)
    local = jnp.sum(jnp.where(valid, jnp.exp(scores - top), 0.0), -1, keepdims=True)
    lse_all[0] = jnp.sum(jnp.where(eye, top + jnp.log(local), 0.0), 0, keepdims=True)
    lse_out = [
        remote(
            lse_all.at[0],
            lse_all.at[dx * 4 + dy],
            lse_sem.at[0],
            lse_sem.at[1],
            **{X: at(X, dx), Y: at(Y, dy)},
        )
        for dx, dy in plane
    ]
    for copy in lse_out:
        copy.start()
    take(lse_all.at[pl.ds(0, 15)], lse_sem.at[1])
    parts = [
        lse_all[lax.rem(x - j // 4 + 4, 4) * 4 + lax.rem(y - j % 4 + 4, 4)] for j in range(16)
    ]
    peak = parts[0]
    for part in parts[1:]:
        peak = jnp.maximum(peak, part)
    mass = jnp.exp(parts[0] - peak)
    for part in parts[1:]:
        mass = mass + jnp.exp(part - peak)
    lse_row = peak + jnp.log(mass)
    lse_ref[...] = lse_row[:, :STATES]
    lse = jnp.sum(jnp.where(eye, lse_row, 0.0), -1, keepdims=True)
    eye_states = lax.broadcasted_iota(jnp.int32, (STATES, STATES), 1) == lax.broadcasted_iota(
        jnp.int32, (STATES, STATES), 0
    )
    target = jnp.sum(jnp.where(eye_states, targets_ref[...], 0.0), -1, keepdims=True)
    data_lane = jnp.where((x == 0) & (y == 0), 0, -1)
    is_data = lane == data_lane
    gap = scores - target
    score_grad[...] = jnp.where(
        valid, penalty_weight * jnp.exp(scores - lse), 0.0
    ) + jnp.where(is_data, gap - penalty_weight, 0.0)
    loss_terms = jnp.where(is_data, penalty_weight * (lse - scores) + 0.5 * gap * gap, 0.0)
    loss_here = jnp.sum(jnp.sum(loss_terms, 0, keepdims=True), -1, keepdims=True)
    loss_here = jnp.where(c == 0, loss_here, 0.0)

    for part, core in ((0, c), (1, other)):
        for i in range(3):
            lines = score_grad[i * (CHUNK // 8) : (i + 1) * (CHUNK // 8), :]
            lines = jnp.broadcast_to(lines[:, None, :], (CHUNK // 8, 8, 128))
            lines = jnp.where((lane8 == row8 + core * 8)[None], lines, 0.0)
            column = jnp.sum(lines.reshape(CHUNK, 128), -1, keepdims=True)
            first = part * ROWS + i * CHUNK
            grad_rows[first : first + CHUNK, :] = jnp.broadcast_to(column, (CHUNK, 128))

    def backward(t, head_sum):
        rows = pl.ds(pl.multiple_of(t * SUB, SUB), SUB)
        g = jnp.concatenate([grad_rows[rows, :]] * (HALF // 128), 1)
        back[rows, :] = (g * slope[rows, :]).astype(BF16)
        return head_sum + jnp.sum((g * head_in[rows, :]).reshape(SUB // 8, 8, HALF), 0)

    head_sum = lax.fori_loop(0, 2 * ROWS // SUB, backward, jnp.zeros((8, HALF), F32), unroll=2)
    vec_x[0, :, :HALF] = jnp.sum(head_sum, 0, keepdims=True)
    vec_x[0, :, HALF:] = jnp.broadcast_to(loss_here, (1, 128))

    def vec_copies(axis, buf, sem, count):
        return [
            remote(buf.at[0], buf.at[d], sem.at[0], sem.at[1], **{axis: at(axis, d)})
            for d in range(1, count)
        ]

    def vec_sum(buf, me, count):
        result = buf[me]
        for q in range(1, count):
            result = result + buf[lax.rem(me - q + count, count)]
        return result

    vec_x_out = vec_copies(X, vec_x, vec_x_sem, 4)
    vec_y_out = vec_copies(Y, vec_y, vec_y_sem, 4)
    vec_z_out = vec_copies(Z, vec_z, vec_z_sem, 8)
    vec_c_out = remote(vec_c.at[0], vec_c.at[1], vec_c_sem.at[0], vec_c_sem.at[1], **{C: other})
    for copy in vec_x_out:
        copy.start()

    def vec_step_y():
        take(vec_x.at[pl.ds(0, 3)], vec_x_sem.at[1])
        vec_y[0] = vec_sum(vec_x, x, 4)
        for copy in vec_y_out:
            copy.start()

    def vec_step_z():
        take(vec_y.at[pl.ds(0, 3)], vec_y_sem.at[1])
        vec_z[0] = vec_sum(vec_y, y, 4)
        for copy in vec_z_out:
            copy.start()

    def vec_step_c():
        take(vec_z.at[pl.ds(0, 7)], vec_z_sem.at[1])
        vec_c[0] = vec_sum(vec_z, z, 8)
        vec_c_out.start()

    def target_z(k):
        return lax.rem(z + jnp.where(lax.rem(k, 2) == 1, 4 - (k + 1) // 2, 4 + k // 2), 8)

    branches = (
        (0, X, Y, x, y, gx, far_x, near_x, mid_x, last_x),
        (1, Y, X, y, x, gy, far_y, near_y, mid_y, last_y),
    )

    def held(n):
        return pl.ds(0, len(GROUPS[n]))

    def far_copies(n, b):
        i, axis, _, me, _, g, far, _, _, _ = branches[b]
        return [
            remote(
                g.at[n, at(axis, 2), pl.ds(2 * s, 2), held(n)],
                far.at[n, s, :, held(n)],
                far_sem.at[i, 0],
                far_sem.at[i, 1 + 2 * n + s],
                **{axis: at(axis, 1 - 2 * s)},
            )
            for s in range(2)
        ]

    def near_copies(n, b):
        i, axis, _, me, _, g, _, near, _, _ = branches[b]
        return [
            remote(
                g.at[n, at(axis, 1 - 2 * s), :, held(n)],
                near.at[n, s, :, held(n)],
                near_sem.at[i, 0],
                near_sem.at[i, 1 + n],
                **{axis: at(axis, 1 - 2 * s)},
            )
            for s in range(2)
        ]

    def mid_copies(n, b):
        i, _, axis, me, _, g, _, _, mid, _ = branches[b]
        return [
            remote(
                g.at[n, me, at(axis, d), held(n)],
                mid.at[n, d - 1, held(n)],
                mid_sem.at[i, 0],
                mid_sem.at[i, 1 + n],
                **{axis: at(axis, d)},
            )
            for d in range(1, 4)
        ]

    def last_copy(k, b):
        i, _, _, me, me2, g, _, _, _, last = branches[b]
        return remote(
            g.at[(k + 1) // 2, me, me2, 0 if k == 0 else (k + 1) % 2],
            last.at[k],
            last_sem.at[i, 0],
            last_sem.at[i, 1],
            **{Z: target_z(k)},
        )

    def block(n, d):
        k = GROUPS[n][0] + d
        columns = pl.ds(pl.multiple_of(target_z(k) * 256, 256), 256)
        result = lax.dot_general(
            normed[:, columns],
            back[...],
            (((0,), (0,)), ((), ())),
            preferred_element_type=F32,
        ).astype(BF16)
        for i in range(4):
            for j in range(4):
                part = result[i * 64 + j * 16 : i * 64 + j * 16 + 16, :]
                gx[n, i, j, d] = part[:, :AHEAD]
                gy[n, j, i, d] = part[:, AHEAD : 2 * AHEAD]
                gz[k, i, j] = part[:, 2 * AHEAD :]

    def stage_block(n):
        def one(d, carry):
            block(n, d)
            return carry

        lax.fori_loop(0, len(GROUPS[n]), one, 0)
        for b in range(2):
            for copy in far_copies(n, b):
                copy.start()

    def stage_near(n):
        for b in range(2):
            _, axis, _, _, _, g, far, _, _, _ = branches[b]
            copies = near_copies(n, b)
            for s, arrived in enumerate(far_copies(n, b)):
                arrived.wait_recv()
                ref = g.at[n, at(axis, 1 - 2 * s), pl.ds(2 * s, 2), held(n)]
                ref[...] = (
                    ref[...].astype(F32) + far[n, s, :, held(n)].astype(F32)
                ).astype(BF16)
                copies[s].start()

    def stage_mid(n):
        for b in range(2):
            _, _, _, me, _, g, _, near, _, _ = branches[b]
            take(near.at[n, :, :, held(n)], near_sem.at[b, 1 + n])
            ref = g.at[n, me, :, held(n)]
            ref[...] = (
                ref[...].astype(F32)
                + near[n, 0, :, held(n)].astype(F32)
                + near[n, 1, :, held(n)].astype(F32)
            ).astype(BF16)
            for copy in mid_copies(n, b):
                copy.start()

    def mid_total(n, b):
        _, _, _, me, me2, g, _, _, mid, _ = branches[b]
        take(mid.at[n, :, held(n)], mid_sem.at[b, 1 + n])
        result = g[n, me, me2, held(n)].astype(F32)
        for d in range(3):
            result = result + mid[n, d, held(n)].astype(F32)
        return result

    def stage_last(n):
        for b in range(2):
            _, _, _, me, me2, g, _, _, _, _ = branches[b]
            g[n, me, me2, held(n)] = mid_total(n, b).astype(BF16)
            for k in GROUPS[n]:
                last_copy(k, b).start()

    far_z_out = [
        remote(
            gz.at[PLUS[4], pl.ds(2 * s, 2)],
            far_z.at[s],
            far_z_sem.at[0],
            far_z_sem.at[1 + s],
            **{Z: at(Z, 1 - 2 * s)},
        )
        for s in range(2)
    ]

    def near_z_copy(j, s, h):
        return remote(
            gz.at[(PLUS, MINUS)[s][j], pl.ds(2 * h, 2)],
            near_z.at[s, j - 1, pl.ds(2 * h, 2)],
            near_z_sem.at[0],
            near_z_sem.at[1 + s * 6 + (j - 1) * 2 + h],
            **{Z: at(Z, 1 - 2 * s)},
        )

    def stage_z(j, late):
        for s in range(2):
            h = s if late else 1 - s
            ref = gz.at[(PLUS, MINUS)[s][j], pl.ds(2 * h, 2)]
            arrived = None
            if j < 3:
                near_z_copy(j + 1, s, h).wait_recv()
                arrived = near_z[s, j, pl.ds(2 * h, 2)]
            elif late:
                far_z_out[s].wait_recv()
                arrived = far_z[s]
            if arrived is not None:
                ref[...] = (ref[...].astype(F32) + arrived.astype(F32)).astype(BF16)
            near_z_copy(j, s, h).start()

    plane_z_out = [
        remote(
            gz.at[7, at(X, dx), at(Y, dy)],
            plane_z.at[dx * 4 + dy],
            plane_z_sem.at[0],
            plane_z_sem.at[1],
            **{X: at(X, dx), Y: at(Y, dy)},
        )
        for dx, dy in plane
    ]

    def stage_z_plane():
        for s in range(2):
            for h in range(2):
                near_z_copy(1, s, h).wait_recv()
        gz[7] = (
            gz[7].astype(F32) + near_z[0, 0].astype(F32) + near_z[1, 0].astype(F32)
        ).astype(BF16)
        for copy in plane_z_out:
            copy.start()

    stage_block(0)
    for copy in far_z_out:
        copy.start()
    stage_block(1)
    stage_z(3, 0)
    stage_block(2)
    vec_step_y()
    stage_near(0)
    stage_z(3, 1)
    stage_block(3)
    stage_block(4)
    stage_near(1)
    stage_z(2, 0)
    stage_near(2)
    stage_z(2, 1)
    stage_mid(0)
    vec_step_z()
    stage_near(3)
    stage_near(4)
    stage_z(1, 0)
    stage_mid(1)
    stage_z(1, 1)
    stage_mid(2)
    stage_last(0)
    vec_step_c()
    stage_mid(3)
    stage_z_plane()
    stage_mid(4)
    stage_last(1)
    stage_last(2)
    stage_last(3)

    for b in range(2):
        total[:, b * AHEAD : (b + 1) * AHEAD] = mid_total(4, b)[0]
    for b in range(2):
        last = branches[b][9]
        result = total[:, b * AHEAD : (b + 1) * AHEAD]
        take(last.at[pl.ds(0, 7)], last_sem.at[b, 1])
        for k in range(7):
            result = result + last[k].astype(F32)
        total[:, b * AHEAD : (b + 1) * AHEAD] = result
    result = gz[7, x, y].astype(F32)
    take(plane_z.at[pl.ds(0, 15)], plane_z_sem.at[1])
    for n in range(1, 16):
        result = result + plane_z[n].astype(F32)
    total[:, 2 * AHEAD :] = result
    total_out = remote(
        total.at[pl.ds(pl.multiple_of(other * 8, 8), 8)],
        total_peer,
        total_sem.at[0],
        total_sem.at[1],
        **{C: other},
    )
    total_out.start()

    vec_c_out.wait_recv()
    grad_head_ref[:, half] = vec_c[0, :, :HALF]
    grad_head_ref[:, other_half] = vec_c[1, :, :HALF]
    loss_ref[...] = (vec_c[0, :, HALF:] + vec_c[1, :, HALF:]) * (1.0 / (STATES * 8))
    grad_ref[:, half] = total[pl.ds(pl.multiple_of(c * 8, 8), 8), :]

    for copy in (pair, scores_out, vec_c_out):
        copy.wait_send()
    for ref, sem in (
        (state_all.at[0, pl.ds(0, 15)], state_sem),
        (lse_all.at[pl.ds(0, 15)], lse_sem),
        (act_buf.at[pl.ds(0, ROWS)], acts_sem),
        (normed.at[pl.ds(0, ROWS)], rows_sem),
        (scale.at[pl.ds(0, ROWS)], scale_sem),
        (vec_x.at[pl.ds(0, 3)], vec_x_sem),
        (vec_y.at[pl.ds(0, 3)], vec_y_sem),
        (vec_z.at[pl.ds(0, 7)], vec_z_sem),
        (gz.at[0], far_z_sem),
        (gz.at[pl.ds(0, 6)], near_z_sem),
        (plane_z.at[pl.ds(0, 15)], plane_z_sem),
    ):
        take(ref, sem.at[0])
    for b in range(2):
        take(gx.at[0], far_sem.at[b, 0])
        take(gx.at[pl.ds(0, 2)], near_sem.at[b, 0])
        take(gx.at[0, pl.ds(0, 3)], mid_sem.at[b, 0])
        take(last_x.at[pl.ds(0, 7)], last_sem.at[b, 0])
    total_out.wait()
    grad_ref[:, other_half] = total_peer[...]


def deliver(grad_in, grad_head_in, lse_in, loss_in, grad_out, grad_head_out, lse_out, loss_out):
    grad_out[...] = grad_in[...]
    grad_head_out[...] = grad_head_in[...]
    lse_out[...] = lse_in[...]
    loss_out[...] = loss_in[:, :1]


def body(state_features, action_features, targets, w_hidden, w_head):
    vmem = pl.BlockSpec(memory_space=pltpu.VMEM)
    anywhere = pl.BlockSpec(memory_space=pl.ANY)
    dma = pltpu.SemaphoreType.DMA
    scratch = [
        pltpu.VMEM((WIDTH, HALF), BF16),
        pltpu.VMEM((2 * ROWS, WIDTH), BF16),
        pltpu.VMEM((64, 128), BF16),
        pltpu.VMEM((2, 16, 64, 128), BF16),
        pltpu.VMEM((STATES, WIDTH), F32),
        pltpu.VMEM((2 * ROWS, WIDTH), BF16),
        pltpu.VMEM((STATES, HALF), F32),
        pltpu.VMEM((2 * ROWS, 128), F32),
        pltpu.VMEM((2 * ROWS, HALF), F32),
        pltpu.VMEM((2 * ROWS, HALF), F32),
        pltpu.VMEM((2 * ROWS, HALF), BF16),
        pltpu.VMEM((2 * ROWS, 128), F32),
        pltpu.VMEM((STATES, 128), F32),
        pltpu.VMEM((STATES, 128), F32),
        pltpu.VMEM((STATES, 128), F32),
        pltpu.VMEM((2 * ROWS, 128), F32),
        pltpu.VMEM((16, 1, 128), F32),
        pltpu.VMEM((4, 1, VECTOR), F32),
        pltpu.VMEM((4, 1, VECTOR), F32),
        pltpu.VMEM((8, 1, VECTOR), F32),
        pltpu.VMEM((2, 1, VECTOR), F32),
        pltpu.VMEM((len(GROUPS), 4, 4, DEPTH, 16, AHEAD), BF16),
        pltpu.VMEM((len(GROUPS), 4, 4, DEPTH, 16, AHEAD), BF16),
        pltpu.VMEM((8, 4, 4, 16, LAST), BF16),
        pltpu.VMEM((len(GROUPS), 2, 2, DEPTH, 16, AHEAD), BF16),
        pltpu.VMEM((len(GROUPS), 2, 2, DEPTH, 16, AHEAD), BF16),
        pltpu.VMEM((len(GROUPS), 2, 4, DEPTH, 16, AHEAD), BF16),
        pltpu.VMEM((len(GROUPS), 2, 4, DEPTH, 16, AHEAD), BF16),
        pltpu.VMEM((len(GROUPS), 3, DEPTH, 16, AHEAD), BF16),
        pltpu.VMEM((len(GROUPS), 3, DEPTH, 16, AHEAD), BF16),
        pltpu.VMEM((8, 16, AHEAD), BF16),
        pltpu.VMEM((8, 16, AHEAD), BF16),
        pltpu.VMEM((2, 2, 4, 16, LAST), BF16),
        pltpu.VMEM((2, 3, 4, 4, 16, LAST), BF16),
        pltpu.VMEM((16, 16, LAST), BF16),
        pltpu.VMEM((16, HALF), F32),
        pltpu.VMEM((8, HALF), F32),
        dma((4,)),
        dma((2,)),
        dma((2,)),
        dma((4,)),
        dma((4,)),
        dma((4,)),
        dma((2,)),
        dma((2,)),
        dma((2,)),
        dma((2,)),
        dma((2,)),
        dma((2,)),
        dma((2, 1 + 2 * len(GROUPS))),
        dma((2, 1 + len(GROUPS))),
        dma((2, 1 + len(GROUPS))),
        dma((2, 2)),
        dma((3,)),
        dma((13,)),
        dma((2,)),
        dma((2,)),
    ]
    grad, grad_head, lse, loss = pl.pallas_call(
        kernel,
        out_shape=(
            jax.ShapeDtypeStruct((8, WIDTH), F32),
            jax.ShapeDtypeStruct((1, WIDTH), F32),
            jax.ShapeDtypeStruct((1, STATES), F32),
            jax.ShapeDtypeStruct((1, 128), F32),
        ),
        in_specs=[vmem, anywhere, vmem, anywhere, vmem],
        out_specs=(vmem,) * 4,
        scratch_shapes=scratch,
        compiler_params=pltpu.CompilerParams(
            collective_id=0, has_side_effects=True, vmem_limit_bytes=52 * 1024 * 1024
        ),
        name="critic",
    )(
        state_features.T,
        action_features.reshape(ROWS, WIDTH),
        targets.reshape(1, STATES),
        w_hidden,
        w_head.reshape(1, WIDTH),
    )
    grad, grad_head, lse, loss = pl.pallas_call(
        deliver,
        out_shape=(
            jax.ShapeDtypeStruct((8, WIDTH), F32),
            jax.ShapeDtypeStruct((1, WIDTH), F32),
            jax.ShapeDtypeStruct((1, STATES), F32),
            jax.ShapeDtypeStruct((1, 1), F32),
        ),
        in_specs=[vmem] * 4,
        out_specs=(vmem,) * 4,
        compiler_params=pltpu.CompilerParams(vmem_limit_bytes=2 * 1024 * 1024),
        name="deliver",
    )(grad, grad_head, lse, loss)
    return grad, grad_head.reshape(WIDTH), lse.reshape(STATES), loss.reshape(())


def solution(mesh):
    finer = Mesh(mesh.devices.reshape(8, 4, 4, 2), (Z, X, Y, C))
    return jax.shard_map(
        body,
        mesh=finer,
        in_specs=(P(Z, ACT), P(Z, ACT, None), P(Z), P(), P()),
        out_specs=(P(STATE_ACT, None), P(), P(Z), P()),
        check_vma=False,
    )
```
